256 devices in a mesh: gx: 16 (over z, y_lo), gy: 16 (over x, y_hi, core).
Axes of the slice: x: 4, y: 4 (y_hi: 2, y_lo: 2; y = y_hi * 2 + y_lo), z: 8, core: 2. Of those that a mesh axis runs over, the one named last changes fastest.
Arguments:
- preserved_vector: float32 [14, 128, 128, 128], P(None, 'gx', 'gy'), may hold values from -200 to 200, as said below
- nasa_table: float32 [32, 6], replicated, may hold values from -4 to 4.5, as said below
- gas_constant: float32 [32], replicated, may hold values from 0.3 to 3
- species_index: int32 [9], replicated, may hold values from 0 to 31, as said below
- face_kind: int32 [16, 16, 2], P('gx', 'gy'), may hold values from 0 to 1
Outputs:
- increment: float32 [14, 128, 128, 128], P(None, 'gx', 'gy')
The draws below stay inside these ranges and needn't reach their ends.
Inputs may be any that keep to these rules, and one draw needn't show every extreme that they name: `preserved_vector`: every cell is a physical state: positive partial densities and an energy whose temperature lies between 0.5 and 2.5. `nasa_table`: each row's cp over R polynomial exceeds 1.5 for temperatures 0.3 to 3. `species_index`: 9 distinct rows.
All inputs are finite; a program needn't handle non-finite values.
Results may differ from the reference program's by a relative error of at most 0.0003.
Values sent between devices are 32-bit elements; how exact they have to be, the bound alone decides.
A program may use at most 64 MiB of HBM per device.

```python
import math
import jax
import jax.numpy as jnp
from jax import lax

NS = 9
NVAR = 14
KINDS = 32
NEWTON = 2
CX = 8
CY = 8
NX = 128
NY = 128
NZ = 128
N_GX = 16
N_GY = 16


def thermo_tables(key):
    lower = jnp.array([2.5, 0.0, -0.05, -0.01, -0.002, -4.0], jnp.float32)
    upper = jnp.array([4.5, 0.6, 0.05, 0.01, 0.002, 4.0], jnp.float32)
    table = lower + (upper - lower) * jax.random.uniform(jax.random.fold_in(key, 101), (KINDS, 6), jnp.float32)
    gases = jnp.exp(jax.random.uniform(jax.random.fold_in(key, 102), (KINDS,), jnp.float32, math.log(0.3), math.log(3.0)))
    middle_rows = (jax.random.permutation(jax.random.fold_in(key, 103), KINDS - 2)[:NS - 2] + 1).astype(jnp.int32)
    end_rows = jnp.array([0, KINDS - 1], jnp.int32)
    pooled = jnp.concatenate([end_rows, middle_rows], axis=0)
    shuffle = jax.random.permutation(jax.random.fold_in(key, 104), NS).astype(jnp.int32)
    chosen = pooled[shuffle].astype(jnp.int32)
    return (table, gases, chosen)


def draw_nasa_table(key, part):
    return thermo_tables(key)[0]


def draw_gas_constant(key, part):
    return thermo_tables(key)[1]


def draw_species_index(key, part):
    return thermo_tables(key)[2]


def draw_preserved_vector(key, part):
    table, gases, chosen = thermo_tables(key)
    nasa_table_weights = table[chosen]
    component_kind_r_factor = gases[chosen]
    grid_sizes_list = (NX, NY, NZ)
    draw_seed_handles_list = [jax.random.fold_in(key, 200 + number) for number in range(6)]
    abscissa_place = (jnp.arange(NX, dtype=jnp.float32) / NX)[:, None, None]
    ordinate_place = (jnp.arange(NY, dtype=jnp.float32) / NY)[None, :, None]
    ramp = 0.3 + 1.35 * (abscissa_place + ordinate_place)
    bulk_compactness = jnp.exp(jax.random.uniform(draw_seed_handles_list[0], grid_sizes_list, jnp.float32, -0.4, 0.4))
    fractions = jax.nn.softmax(jax.random.normal(draw_seed_handles_list[1], (NS,) + grid_sizes_list, jnp.float32), axis=0)
    passive = jax.random.uniform(draw_seed_handles_list[2], grid_sizes_list, jnp.float32)
    kelvin_reading = jax.random.uniform(draw_seed_handles_list[3], grid_sizes_list, jnp.float32, 0.5, 2.4)
    velocity = 0.5 * ramp[None] * jnp.clip(jax.random.normal(draw_seed_handles_list[4], (3,) + grid_sizes_list, jnp.float32), -4.0, 4.0)
    prefix_addition_result = bulk_compactness[None] * fractions
    replicated_layer = kelvin_reading[None]
    columns = [nasa_table_weights[:, degree].reshape((NS, 1, 1, 1)) for degree in range(6)]
    chemical_heat_content = columns[5] + replicated_layer * (columns[0] + replicated_layer * (columns[1] / 2.0 + replicated_layer * (columns[2] / 3.0 + replicated_layer * (columns[3] / 4.0 + replicated_layer * columns[4] / 5.0))))
    caloric_tiers = component_kind_r_factor.reshape((NS, 1, 1, 1)) * (chemical_heat_content - replicated_layer)
    energy = jnp.sum(prefix_addition_result * caloric_tiers, axis=0) + 0.5 * bulk_compactness * jnp.sum(velocity * velocity, axis=0)
    return jnp.concatenate([prefix_addition_result, bulk_compactness[None] * velocity, energy[None], (bulk_compactness * passive)[None]], axis=0).astype(jnp.float32)


def set_ends(values, key, least, high):
    dims = values.shape
    index_at = [jax.random.randint(jax.random.fold_in(key, axis), (), 0, dims[axis]) for axis in range(len(dims))]
    values = values.at[tuple(index_at)].set(least)
    longest = dims.index(max(dims))
    index_at[longest] = (index_at[longest] + 1) % dims[longest]
    return values.at[tuple(index_at)].set(high)


def setup_inputs(seed: int = 0) -> dict:
    arg_keys = jax.random.split(jax.random.key(seed), 6)
    preserved_vector = draw_preserved_vector(jax.random.fold_in(arg_keys[5], 71), 0)
    nasa_table = draw_nasa_table(jax.random.fold_in(arg_keys[5], 71), 0)
    gas_constant = draw_gas_constant(jax.random.fold_in(arg_keys[5], 71), 0)
    species_index = draw_species_index(jax.random.fold_in(arg_keys[5], 71), 0)
    face_kind = set_ends(jax.random.randint(arg_keys[4], (N_GX, N_GY, 2), 0, 2), jax.random.fold_in(arg_keys[4], 1), 0, 1).astype(jnp.int32)
    return {"preserved_vector": preserved_vector, "nasa_table": nasa_table, "gas_constant": gas_constant, "species_index": species_index, "face_kind": face_kind}


EPSILON = 1e-06
COURANT = 0.8

def column(vector, trailing_sizes):
    return vector.reshape((vector.shape[0],) + (1,) * trailing_sizes)

def caloric_fitted_curves_table(nasa_table_weights, kelvin_reading):
    trailing_sizes = kelvin_reading.ndim
    columns = [column(nasa_table_weights[:, degree], trailing_sizes) for degree in range(6)]
    replicated_layer = kelvin_reading[None]
    caloric_quotient = columns[0] + replicated_layer * (columns[1] + replicated_layer * (columns[2] + replicated_layer * (columns[3] + replicated_layer * columns[4])))
    chemical_heat_content = columns[5] + replicated_layer * (columns[0] + replicated_layer * (columns[1] / 2.0 + replicated_layer * (columns[2] / 3.0 + replicated_layer * (columns[3] / 4.0 + replicated_layer * columns[4] / 5.0))))
    return (caloric_quotient, chemical_heat_content)

def solve_for_kelvin(preserved_vector_lines, nasa_table_weights, component_kind_r_factor):
    prefix_addition_result = preserved_vector_lines[:NS]
    bulk_compactness = lax.optimization_barrier(jnp.sum(prefix_addition_result, axis=0))
    momentum = preserved_vector_lines[NS:NS + 3]
    caloric_content_inner = preserved_vector_lines[NS + 3] - 0.5 * lax.optimization_barrier(jnp.sum(momentum * momentum, axis=0)) / bulk_compactness
    blend_stack_lane = column(component_kind_r_factor, bulk_compactness.ndim)
    kelvin_reading = jnp.ones_like(bulk_compactness)
    for iteration in range(NEWTON):
        caloric_quotient, chemical_heat_content = caloric_fitted_curves_table(nasa_table_weights, kelvin_reading)
        solver_misfit = lax.optimization_barrier(jnp.sum(prefix_addition_result * blend_stack_lane * (chemical_heat_content - kelvin_reading[None]), axis=0)) - caloric_content_inner
        tangent_steepness_fn = lax.optimization_barrier(jnp.sum(prefix_addition_result * blend_stack_lane * (caloric_quotient - 1.0), axis=0))
        kelvin_reading = kelvin_reading - solver_misfit / tangent_steepness_fn
    return kelvin_reading

def nasa_fitted_monomials(preserved_vector_lines, kelvin_reading, nasa_table_weights, component_kind_r_factor):
    prefix_addition_result = preserved_vector_lines[:NS]
    bulk_compactness = lax.optimization_barrier(jnp.sum(prefix_addition_result, axis=0))
    momentum = preserved_vector_lines[NS:NS + 3]
    doubled_norm_motion = lax.optimization_barrier(jnp.sum(momentum * momentum, axis=0)) / (bulk_compactness * bulk_compactness)
    blend_stack_lane = column(component_kind_r_factor, bulk_compactness.ndim)
    caloric_quotient, chemical_heat_content = caloric_fitted_curves_table(nasa_table_weights, kelvin_reading)
    caloric_tiers = blend_stack_lane * (chemical_heat_content - kelvin_reading[None])
    averaged_mixing_law_r = lax.optimization_barrier(jnp.sum(prefix_addition_result * blend_stack_lane, axis=0))
    thrust_load_quiet = averaged_mixing_law_r * kelvin_reading
    heat_quotient_decrement = averaged_mixing_law_r / lax.optimization_barrier(jnp.sum(prefix_addition_result * blend_stack_lane * (caloric_quotient - 1.0), axis=0))
    sound_speed = jnp.sqrt((1.0 + heat_quotient_decrement) * thrust_load_quiet / bulk_compactness)
    force_spatial_jump = blend_stack_lane * kelvin_reading[None] - heat_quotient_decrement[None] * caloric_tiers + 0.5 * heat_quotient_decrement[None] * doubled_norm_motion[None]
    return jnp.concatenate([thrust_load_quiet[None], heat_quotient_decrement[None], sound_speed[None], force_spatial_jump], axis=0)

def reconstruct(values):
    value_zero, value_one, value_two, value_three, value_four = values
    candidate_zero = (2.0 * value_zero - 7.0 * value_one + 11.0 * value_two) / 6.0
    candidate_one = (-value_one + 5.0 * value_two + 2.0 * value_three) / 6.0
    candidate_two = (2.0 * value_two + 5.0 * value_three - value_four) / 6.0
    curve_zero = value_zero - 2.0 * value_one + value_two
    slope_zero = value_zero - 4.0 * value_one + 3.0 * value_two
    curve_one = value_one - 2.0 * value_two + value_three
    slope_one = value_one - value_three
    curve_two = value_two - 2.0 * value_three + value_four
    slope_two = 3.0 * value_two - 4.0 * value_three + value_four
    smooth_zero = 13.0 / 12.0 * curve_zero * curve_zero + 0.25 * slope_zero * slope_zero
    smooth_one = 13.0 / 12.0 * curve_one * curve_one + 0.25 * slope_one * slope_one
    smooth_two = 13.0 / 12.0 * curve_two * curve_two + 0.25 * slope_two * slope_two
    weight_zero = 0.1 / ((EPSILON + smooth_zero) * (EPSILON + smooth_zero))
    weight_one = 0.6 / ((EPSILON + smooth_one) * (EPSILON + smooth_one))
    weight_two = 0.3 / ((EPSILON + smooth_two) * (EPSILON + smooth_two))
    return (weight_zero * candidate_zero + weight_one * candidate_one + weight_two * candidate_two) / (weight_zero + weight_one + weight_two)

def window(array, offset, count, array_axis):
    return lax.slice_in_dim(array, offset, offset + count, axis=array_axis)

def direction_rate(preserved_vector_lines, cell_coef, array_axis, normal, speed):
    cells = preserved_vector_lines.shape[array_axis] - 6
    faces = cells + 1
    bulk_compactness = lax.optimization_barrier(jnp.sum(preserved_vector_lines[:NS], axis=0))
    fractions = preserved_vector_lines[:NS] / bulk_compactness[None]
    velocity = preserved_vector_lines[NS:NS + 3] / bulk_compactness[None]
    passive = preserved_vector_lines[NS + 4:NS + 5] / bulk_compactness[None]
    thrust_load_quiet = cell_coef[0]
    normal_speed = velocity[normal]
    carried = preserved_vector_lines * normal_speed[None]
    flux_rows = [carried[:NS]]
    for component in range(3):
        if component == normal:
            flux_rows.append((carried[NS + component] + thrust_load_quiet)[None])
        else:
            flux_rows.append(carried[NS + component][None])
    flux_rows.append((carried[NS + 3] + thrust_load_quiet * normal_speed)[None])
    flux_rows.append(carried[NS + 4][None])
    physical = jnp.concatenate(flux_rows, axis=0)
    upwind = 0.5 * (physical + speed * preserved_vector_lines)
    downwind = 0.5 * (physical - speed * preserved_vector_lines)

    def average(array):
        return 0.5 * (window(array, 2, faces, array_axis) + window(array, 3, faces, array_axis))
    mean_frac = average(fractions)
    mean_vel = average(velocity)
    mean_passive = average(passive)[0]
    mean_gamma = average(cell_coef[1:2])[0]
    mean_sound = average(cell_coef[2:3])[0]
    mean_slopes = average(cell_coef[3:])
    mean_square = lax.optimization_barrier(jnp.sum(mean_vel * mean_vel, axis=0))
    mean_enthalpy = (mean_sound * mean_sound - lax.optimization_barrier(jnp.sum(mean_frac * mean_slopes, axis=0))) / mean_gamma + mean_square
    inverse = 1.0 / (mean_sound * mean_sound)
    tangents = [component for component in range(3) if component != normal]

    def project(vector):
        total = lax.optimization_barrier(jnp.sum(vector[:NS], axis=0))
        pressure_jump = lax.optimization_barrier(jnp.sum(mean_slopes * vector[:NS], axis=0)) - mean_gamma * lax.optimization_barrier(jnp.sum(mean_vel * vector[NS:NS + 3], axis=0)) + mean_gamma * vector[NS + 3]
        normal_jump = vector[NS + normal] - mean_vel[normal] * total
        scaled = pressure_jump * inverse
        slower = 0.5 * (pressure_jump - mean_sound * normal_jump) * inverse
        faster = 0.5 * (pressure_jump + mean_sound * normal_jump) * inverse
        species = vector[:NS] - mean_frac * scaled[None]
        first_shear = vector[NS + tangents[0]] - mean_vel[tangents[0]] * total
        second_shear = vector[NS + tangents[1]] - mean_vel[tangents[1]] * total
        scalar_wave = vector[NS + 4] - mean_passive * scaled
        return jnp.concatenate([slower[None], species, first_shear[None], second_shear[None], faster[None], scalar_wave[None]], axis=0)
    rising = reconstruct([project(window(upwind, offset, faces, array_axis)) for offset in (0, 1, 2, 3, 4)])
    falling = reconstruct([project(window(downwind, offset, faces, array_axis)) for offset in (5, 4, 3, 2, 1)])
    amplitude = rising + falling
    slower = amplitude[0]
    species = amplitude[1:NS + 1]
    first_shear = amplitude[NS + 1]
    second_shear = amplitude[NS + 2]
    faster = amplitude[NS + 3]
    scalar_wave = amplitude[NS + 4]
    species_total = lax.optimization_barrier(jnp.sum(species, axis=0))
    acoustic = slower + faster
    normal_vel = mean_vel[normal]
    momentum_rows = []
    for component in range(3):
        if component == normal:
            momentum_rows.append((normal_vel - mean_sound) * slower + (normal_vel + mean_sound) * faster + normal_vel * species_total)
        elif component == tangents[0]:
            momentum_rows.append(mean_vel[component] * (acoustic + species_total) + first_shear)
        else:
            momentum_rows.append(mean_vel[component] * (acoustic + species_total) + second_shear)
    energy_row = (mean_enthalpy - normal_vel * mean_sound) * slower + (mean_enthalpy + normal_vel * mean_sound) * faster + lax.optimization_barrier(jnp.sum((mean_square[None] - mean_slopes / mean_gamma[None]) * species, axis=0)) + mean_vel[tangents[0]] * first_shear + mean_vel[tangents[1]] * second_shear
    face_flux = jnp.concatenate([mean_frac * acoustic[None] + species, jnp.stack(momentum_rows, axis=0), energy_row[None], (mean_passive * acoustic + scalar_wave)[None]], axis=0)
    return window(face_flux, 0, cells, array_axis) - window(face_flux, 1, cells, array_axis)

def wall_pad(payload, lower_kind, upper_kind):
    rows_count = payload.shape[0]
    sign_flips = jnp.where(jnp.arange(rows_count) == NS + 2, -1.0, 1.0).astype(payload.dtype).reshape((rows_count, 1, 1, 1))
    lower_copy = jnp.concatenate([payload[..., :1]] * 3, axis=3)
    upper_copy = jnp.concatenate([payload[..., -1:]] * 3, axis=3)
    lower_mirror = payload[..., 2::-1] * sign_flips
    upper_mirror = payload[..., :-4:-1] * sign_flips
    lower_ghost = jnp.where(lower_kind == 1, lower_mirror, lower_copy)
    upper_ghost = jnp.where(upper_kind == 1, upper_mirror, upper_copy)
    return jnp.concatenate([lower_ghost, payload, upper_ghost], axis=3)

def reference(preserved_vector, nasa_table, gas_constant, species_index, face_kind):
    nasa_table_weights = nasa_table[species_index]
    component_kind_r_factor = gas_constant[species_index]
    block_ids = jnp.arange(N_GX, dtype=jnp.int32)

    def cell_block(block_id):
        patch_region = lax.dynamic_slice_in_dim(preserved_vector, (block_id * CX).astype(jnp.int32), CX, 1)
        kelvin_reading = solve_for_kelvin(patch_region, nasa_table_weights, component_kind_r_factor)
        patch_multiplier = nasa_fitted_monomials(patch_region, kelvin_reading, nasa_table_weights, component_kind_r_factor)
        bulk_compactness = lax.optimization_barrier(jnp.sum(patch_region[:NS], axis=0))
        velocity = patch_region[NS:NS + 3] / bulk_compactness[None]
        local_speed = lax.optimization_barrier(jnp.max(jnp.abs(velocity) + patch_multiplier[2][None], axis=(1, 2, 3)))
        return (patch_multiplier, local_speed)
    coef_blocks, speed_blocks = lax.map(cell_block, block_ids)
    cell_coef = jnp.transpose(coef_blocks, (1, 0, 2, 3, 4)).reshape((NS + 3, NX, NY, NZ))
    speeds = lax.optimization_barrier(jnp.max(speed_blocks, axis=0))

    def rate_block(inputs):
        block_id, kinds = inputs
        rows_index = (block_id * CX - 3 + jnp.arange(CX + 6, dtype=jnp.int32)) % NX
        state_x = jnp.take(preserved_vector, rows_index, axis=1)
        coef_x = jnp.take(cell_coef, rows_index, axis=1)
        rate = direction_rate(state_x, coef_x, 1, 0, speeds[0])
        state_mid = state_x[:, 3:3 + CX]
        coef_mid = coef_x[:, 3:3 + CX]
        state_y = jnp.concatenate([state_mid[:, :, -3:], state_mid, state_mid[:, :, :3]], axis=2)
        coef_y = jnp.concatenate([coef_mid[:, :, -3:], coef_mid, coef_mid[:, :, :3]], axis=2)
        rate = rate + direction_rate(state_y, coef_y, 2, 1, speeds[1])
        lower_kind = jnp.repeat(kinds[:, 0], CY).reshape((1, 1, NY, 1))
        upper_kind = jnp.repeat(kinds[:, 1], CY).reshape((1, 1, NY, 1))
        padded_z = wall_pad(jnp.concatenate([state_mid, coef_mid], axis=0), lower_kind, upper_kind)
        rate = rate + direction_rate(padded_z[:NVAR], padded_z[NVAR:], 3, 2, speeds[2])
        return rate
    rate_blocks = lax.map(rate_block, (block_ids, face_kind))
    rate = jnp.transpose(rate_blocks, (1, 0, 2, 3, 4)).reshape((NVAR, NX, NY, NZ))
    return COURANT / jnp.sum(speeds) * rate
```

```python
import functools

import jax
import jax.numpy as jnp
from jax import lax
from jax.experimental import pallas as pl
from jax.experimental.pallas import tpu as pltpu
from jax.sharding import PartitionSpec as P

NS = 9
NVAR = 14
NEWTON = 2
EPSILON = 1e-06
COURANT = 0.8
KX, KY, KZ = 3, 3, 3

ROWS = 14
FACES = 9
ORDER = (
    tuple(range(9)) + (9, 10, 11, 12, 13),
    tuple(range(9)) + (10, 9, 11, 12, 13),
    tuple(range(9)) + (11, 9, 10, 12, 13),
)
NM = 9
T1, T2, EN, SC = 10, 11, 12, 13
CY, CU, CZ, CG, CC, CPHI, CP, CRHO = 0, 9, 12, 13, 14, 15, 24, 25
NCELL = 26
NFLUX = 15


def fill_table(nasa_ref, gas_ref, index_ref, tab_ref):
    for i in range(NS):
        k = index_ref[i]
        r = gas_ref[k]
        a = [nasa_ref[k, n] for n in range(6)]
        tab_ref[i, 0] = r
        tab_ref[i, 1] = r * (a[0] - 1.0)
        tab_ref[i, 2] = r * a[1]
        tab_ref[i, 3] = r * a[2]
        tab_ref[i, 4] = r * a[3]
        tab_ref[i, 5] = r * a[4]
        tab_ref[i, 6] = r * a[5]
        tab_ref[i, 7] = r * a[1] * 0.5
        tab_ref[i, 8] = r * a[2] * (1.0 / 3.0)
        tab_ref[i, 9] = r * a[3] * 0.25
        tab_ref[i, 10] = r * a[4] * 0.2


def cell_row(u, tab_ref):
    rho = u[0]
    for i in range(1, NS):
        rho = rho + u[i]
    inv = 1.0 / rho
    square = u[NM] * u[NM] + u[T1] * u[T1] + u[T2] * u[T2]
    energy = u[EN] - 0.5 * square * inv
    moment = []
    for n in range(7):
        total = u[0] * tab_ref[0, n]
        for i in range(1, NS):
            total = total + u[i] * tab_ref[i, n]
        moment.append(total)
    gas, k1, k2, k3, k4, k5, k6 = moment
    l2, l3, l4, l5 = k2 * 0.5, k3 * (1.0 / 3.0), k4 * 0.25, k5 * 0.2
    base = k6 - energy
    t = 1.0
    for _ in range(NEWTON):
        f = base + t * (k1 + t * (l2 + t * (l3 + t * (l4 + t * l5))))
        slope = k1 + t * (k2 + t * (k3 + t * (k4 + t * k5)))
        t = t - f / slope
    heat = k1 + t * (k2 + t * (k3 + t * (k4 + t * k5)))
    g = gas / heat
    p = gas * t
    c = jnp.sqrt((1.0 + g) * p * inv)
    half_q = 0.5 * square * inv * inv
    half_g, half_t = 0.5 * g, 0.5 * t
    phi = []
    for i in range(NS):
        e = tab_ref[i, 6] + t * (
            tab_ref[i, 1]
            + t * (tab_ref[i, 7] + t * (tab_ref[i, 8] + t * (tab_ref[i, 9] + t * tab_ref[i, 10])))
        )
        phi.append(tab_ref[i, 0] * half_t - half_g * (e - half_q))
    half_inv = 0.5 * inv
    cell = [u[i] * inv for i in range(NS)]
    cell += [u[k] * half_inv for k in (NM, T1, T2)]
    cell += [u[SC] * inv, half_g, 0.5 * c] + phi + [p, rho]
    speed = [jnp.abs(u[k] * inv) + c for k in (NM, T1, T2)]
    return cell, speed


def flux_rows(u, half_v, p, rho, alpha):
    v = half_v + half_v
    plus, minus = [], []
    for k in range(NVAR):
        if k == EN:
            f = (u[k] + p) * v
        elif k == NM:
            f = u[k] * v + p
        else:
            f = u[k] * v
        a = alpha * u[k]
        plus.append(f + a)
        minus.append(f - a)
    a = alpha * rho
    plus.append(u[NM] + a)
    minus.append(u[NM] - a)
    return plus, minus


def weno(d0, d1, d2, d3):
    eps = 3.0 * EPSILON
    a1, a2 = d1 * d1, d2 * d2
    s0 = d0 * (d0 - 2.75 * d1) + (2.5 * a1 + eps)
    s2 = d3 * (d3 - 2.75 * d2) + (2.5 * a2 + eps)
    s1 = (a1 - 1.25 * (d1 * d2)) + (a2 + eps)
    r0, r1, r2 = 1.0 / s0, 1.0 / s1, 1.0 / s2
    w0, w1, w2 = r0 * r0, r1 * r1, 3.0 * (r2 * r2)
    c0, c1, c2 = d1 - d0, d2 - d1, d3 - d2
    x0 = w0 * (c1 - c0)
    number = (x0 + x0) + w2 * (c2 - c1)
    total = (w0 + w2) + 6.0 * w1
    return ((d1 + d2) + d2) - number / total


def face_row(cell, diff, base):
    low, high = cell
    mean = [low[n] + high[n] for n in range(CP)]
    y = mean[CY : CY + NS]
    vn, v1, v2 = mean[CU : CU + 3]
    z, g, c = mean[CZ], mean[CG], mean[CC]
    phi = mean[CPHI : CPHI + NS]
    half_over_c = 0.5 / c
    half_over_cc = 2.0 * half_over_c * half_over_c

    def split(d):
        dp = phi[0] * d[0]
        for i in range(1, NS):
            dp = dp + phi[i] * d[i]
        work = vn * d[NM] + v1 * d[T1] + v2 * d[T2]
        dp = dp + g * (d[EN] - work)
        total = d[NVAR]
        a = dp * half_over_cc
        b = (d[NM] - vn * total) * half_over_c
        return a, a - b, a + b, d[T1] - v1 * total, d[T2] - v2 * total, d[SC] - z * a

    parts = [split(d) for d in diff]

    def both(values):
        return weno(*values[:4]) - weno(*values[4:])

    slow, fast, shear1, shear2, scalar = [both([p[n] for p in parts]) for n in range(1, 6)]
    species = [both([d[i] - y[i] * p[0] for d, p in zip(diff, parts)]) for i in range(NS)]
    acoustic = slow + fast
    half_acoustic = 0.5 * acoustic
    pull = c * (fast - slow)
    total = species[0]
    for i in range(1, NS):
        total = total + species[i]
    carried = acoustic + total
    weight = c * c - 0.5 * functools.reduce(lambda s, i: s + y[i] * phi[i], range(1, NS), y[0] * phi[0])
    heat = functools.reduce(lambda s, i: s + species[i] * phi[i], range(1, NS), species[0] * phi[0])
    square = vn * vn + v1 * v1 + v2 * v2
    energy = (
        (weight * acoustic - heat) / g
        + square * carried
        + vn * pull
        + v1 * shear1
        + v2 * shear2
    )
    rows = [species[i] + y[i] * half_acoustic for i in range(NS)]
    rows += [vn * carried + pull, v1 * carried + shear1, v2 * carried + shear2, energy]
    rows += [z * half_acoustic + scalar]
    return [6.0 * base[k] + rows[k] for k in range(NVAR)]


def compute_kernel(
    u_ref, xl_ref, xh_ref, yl_ref, yh_ref, alpha_ref, nasa_ref, gas_ref, index_ref, kind_ref, out_ref,
    tab, uq, cq, ps, ms, dp, dm, fx, tmp,
):
    fill_table(nasa_ref, gas_ref, index_ref, tab)
    lane = lax.broadcasted_iota(jnp.int32, (8, 128), 1)
    sub = lax.broadcasted_iota(jnp.int32, (8, 128), 0)
    left = lane < 64

    for k in range(NVAR):
        cx, cy = ORDER[0][k], ORDER[1][k]
        for r in range(8):
            uq[3 + r, k] = u_ref[cx, 8 * r : 8 * r + 8, :]
            uq[ROWS + 3 + r, k] = u_ref[cy, pl.ds(r, 8, stride=8), :]
        for r in range(3):
            uq[r, k] = xl_ref[cx, r]
            uq[11 + r, k] = xh_ref[cx, r]
            uq[ROWS + r, k] = yl_ref[cy, r]
            uq[ROWS + 11 + r, k] = yh_ref[cy, r]
    zb = 2 * ROWS
    for pair in range(NVAR // 2):
        a, b = 2 * pair, 2 * pair + 1
        both = jnp.concatenate([u_ref[a], u_ref[b]], axis=0)
        turned = jnp.transpose(both)
        for t in range(8):
            lo, hi = turned[8 * t : 8 * t + 8], turned[64 + 8 * t : 72 + 8 * t]
            tmp[a, 8 * t : 8 * t + 8, :] = jnp.where(left, lo, pltpu.roll(hi, 64, 1))
            tmp[b, 8 * t : 8 * t + 8, :] = jnp.where(left, pltpu.roll(lo, 64, 1), hi)
    low_kind, high_kind = kind_ref[0, 0, 0], kind_ref[0, 0, 1]
    low_wall, high_wall = (low_kind == 1), (high_kind == 1)
    for k in range(NVAR):
        cz = ORDER[2][k]
        rows = [tmp[cz, pl.ds(l, 8, stride=8), :] for l in range(8)]
        for l in range(8):
            uq[zb + 3 + l, k] = rows[l]
        sign = -1.0 if k == NM else 1.0
        for n in range(3):
            inside = pltpu.roll(rows[7 - n], 1, 0)
            ghost = jnp.where(low_wall, sign * rows[n], rows[0])
            edge = jnp.where(left, ghost, pltpu.roll(inside, 64, 1))
            uq[zb + 2 - n, k] = jnp.where(sub == 0, edge, inside)
            inside = pltpu.roll(rows[n], 7, 0)
            ghost = jnp.where(high_wall, sign * rows[7 - n], rows[7])
            edge = jnp.where(left, pltpu.roll(inside, 64, 1), ghost)
            uq[zb + 11 + n, k] = jnp.where(sub == 7, edge, inside)

    @pl.loop(0, 3 * ROWS)
    def _(r):
        cell, _ = cell_row([uq[r, k] for k in range(NVAR)], tab)
        for n in range(NCELL):
            cq[r, n] = cell[n]

    @pl.loop(0, 3)
    def _(d):
        first = d * ROWS
        alpha = alpha_ref[d]

        @pl.loop(0, ROWS)
        def _(r):
            plus, minus = flux_rows(
                [uq[first + r, k] for k in range(NVAR)],
                cq[first + r, CU], cq[first + r, CP], cq[first + r, CRHO], alpha,
            )
            for k in range(NFLUX):
                ps[r, k] = plus[k]
                ms[r, k] = minus[k]

        @pl.loop(0, ROWS - 1)
        def _(r):
            for k in range(NFLUX):
                dp[r, k] = ps[r + 1, k] - ps[r, k]
                dm[r, k] = ms[r + 1, k] - ms[r, k]

        @pl.loop(0, FACES)
        def _(f):
            diff = [[dp[f + n, k] for k in range(NFLUX)] for n in (0, 1, 2, 3)]
            diff += [[dm[f + n, k] for k in range(NFLUX)] for n in (4, 3, 2, 1)]
            base = [ps[f + 2, k] + ms[f + 3, k] for k in range(NVAR)]
            cell = [[cq[first + f + n, k] for k in range(CP)] for n in (2, 3)]
            flux = face_row(cell, diff, base)
            for k in range(NVAR):
                fx[d * FACES + f, k] = flux[k]

    scale = (COURANT / 12.0) / (alpha_ref[0] + alpha_ref[1] + alpha_ref[2])
    for k in range(NVAR):
        for r in range(8):
            tmp[ORDER[1][k], 8 * r : 8 * r + 8, :] = fx[FACES + r, k] - fx[FACES + r + 1, k]
    for k in range(NVAR):
        for r in range(8):
            rate = (fx[r, k] - fx[r + 1, k]) + tmp[k, pl.ds(r, 8, stride=8), :]
            out_ref[k, 8 * r : 8 * r + 8, :] = rate
    for k in range(NVAR):
        for r in range(8):
            tmp[ORDER[2][k], 8 * r : 8 * r + 8, :] = fx[2 * FACES + r, k] - fx[2 * FACES + r + 1, k]
    for pair in range(NVAR // 2):
        a, b = 2 * pair, 2 * pair + 1
        low, high = [], []
        for t in range(8):
            ra = tmp[a, pl.ds(t, 8, stride=8), :]
            rb = tmp[b, pl.ds(t, 8, stride=8), :]
            low.append(jnp.where(left, ra, pltpu.roll(rb, 64, 1)))
            high.append(jnp.where(left, pltpu.roll(ra, 64, 1), rb))
        back = jnp.transpose(jnp.concatenate(low + high, axis=0))
        out_ref[a] = scale * (out_ref[a] + back[:64])
        out_ref[b] = scale * (out_ref[b] + back[64:])


def compute(u, halos, alpha, nasa, gas, index, kind):
    vmem = pl.BlockSpec(memory_space=pltpu.VMEM)
    smem = pl.BlockSpec(memory_space=pltpu.SMEM)
    f32 = jnp.float32
    return pl.pallas_call(
        compute_kernel,
        out_shape=jax.ShapeDtypeStruct((NVAR, 64, 128), f32),
        in_specs=[vmem] * 5 + [smem] * 5,
        out_specs=vmem,
        scratch_shapes=[
            pltpu.SMEM((NS, 11), f32),
            pltpu.VMEM((3 * ROWS, NVAR, 8, 128), f32),
            pltpu.VMEM((3 * ROWS, NCELL, 8, 128), f32),
            pltpu.VMEM((ROWS, NFLUX, 8, 128), f32),
            pltpu.VMEM((ROWS, NFLUX, 8, 128), f32),
            pltpu.VMEM((ROWS, NFLUX, 8, 128), f32),
            pltpu.VMEM((ROWS, NFLUX, 8, 128), f32),
            pltpu.VMEM((3 * FACES, NVAR, 8, 128), f32),
            pltpu.VMEM((NVAR, 64, 128), f32),
        ],
    )(u, *halos, alpha, nasa, gas, index, kind)


def local_speeds(u, nasa, gas, index):
    def kernel(u_ref, nasa_ref, gas_ref, index_ref, out_ref, tab):
        fill_table(nasa_ref, gas_ref, index_ref, tab)
        best = None
        for r in range(8):
            _, speed = cell_row([u_ref[k, 8 * r : 8 * r + 8, :] for k in range(NVAR)], tab)
            best = speed if best is None else [jnp.maximum(a, b) for a, b in zip(best, speed)]
        for d in range(3):
            out_ref[d] = best[d]

    vmem = pl.BlockSpec(memory_space=pltpu.VMEM)
    smem = pl.BlockSpec(memory_space=pltpu.SMEM)
    best = pl.pallas_call(
        kernel,
        out_shape=jax.ShapeDtypeStruct((3, 8, 128), jnp.float32),
        in_specs=[vmem] + [smem] * 3,
        out_specs=vmem,
        scratch_shapes=[pltpu.SMEM((NS, 11), jnp.float32)],
    )(u, nasa, gas, index)
    return jnp.max(best, axis=(1, 2))


def solution(mesh):
    def shards(u, nasa, gas, index, kind):
        flat = u.reshape(NVAR, 64, 128)
        alpha = lax.pmax(local_speeds(flat, nasa, gas, index), ("gx", "gy"))
        halos = []
        for axis, dim in (("gx", 1), ("gy", 2)):
            n = mesh.shape[axis]
            up = [(i, (i + 1) % n) for i in range(n)]
            for piece, pairs in (
                (lax.slice_in_dim(u, 5, 8, axis=dim), up),
                (lax.slice_in_dim(u, 0, 3, axis=dim), [(b, a) for a, b in up]),
            ):
                if dim == 2:
                    piece = jnp.swapaxes(piece, 1, 2)
                halos.append(lax.ppermute(piece, axis, pairs))
        out = compute(flat, halos, alpha, nasa, gas, index, kind)
        return out.reshape(u.shape)

    whole = P(None, "gx", "gy", None)
    return jax.shard_map(
        shards, mesh=mesh, in_specs=(whole, P(), P(), P(), P("gx", "gy", None)), out_specs=whole, check_vma=False
    )
```

```python
import functools

import jax
import jax.numpy as jnp
from jax import lax
from jax.experimental import pallas as pl
from jax.experimental.pallas import tpu as pltpu
from jax.sharding import PartitionSpec as P

NS = 9
NVAR = 14
NEWTON = 2
EPSILON = 1e-06
COURANT = 0.8
KX, KY, KZ = 3, 3, 3

ROWS = 14
FACES = 9
ORDER = (
    tuple(range(9)) + (9, 10, 11, 12, 13),
    tuple(range(9)) + (10, 9, 11, 12, 13),
    tuple(range(9)) + (11, 9, 10, 12, 13),
)
NM = 9
T1, T2, EN, SC = 10, 11, 12, 13
CY, CU, CZ, CG, CC, CPHI, CP, CRHO = 0, 9, 12, 13, 14, 15, 24, 25
NCELL = 26
NFLUX = 15


def fill_table(nasa_ref, gas_ref, index_ref, tab_ref):
    for i in range(NS):
        k = index_ref[i]
        r = gas_ref[k]
        a = [nasa_ref[k, n] for n in range(6)]
        tab_ref[i, 0] = r
        tab_ref[i, 1] = r * (a[0] - 1.0)
        tab_ref[i, 2] = r * a[1]
        tab_ref[i, 3] = r * a[2]
        tab_ref[i, 4] = r * a[3]
        tab_ref[i, 5] = r * a[4]
        tab_ref[i, 6] = r * a[5]
        tab_ref[i, 7] = r * a[1] * 0.5
        tab_ref[i, 8] = r * a[2] * (1.0 / 3.0)
        tab_ref[i, 9] = r * a[3] * 0.25
        tab_ref[i, 10] = r * a[4] * 0.2


def cell_row(u, tab_ref):
    rho = u[0]
    for i in range(1, NS):
        rho = rho + u[i]
    inv = 1.0 / rho
    square = u[NM] * u[NM] + u[T1] * u[T1] + u[T2] * u[T2]
    energy = u[EN] - 0.5 * square * inv
    moment = []
    for n in range(7):
        total = u[0] * tab_ref[0, n]
        for i in range(1, NS):
            total = total + u[i] * tab_ref[i, n]
        moment.append(total)
    gas, k1, k2, k3, k4, k5, k6 = moment
    l2, l3, l4, l5 = k2 * 0.5, k3 * (1.0 / 3.0), k4 * 0.25, k5 * 0.2
    base = k6 - energy
    t = 1.0
    for _ in range(NEWTON):
        f = base + t * (k1 + t * (l2 + t * (l3 + t * (l4 + t * l5))))
        slope = k1 + t * (k2 + t * (k3 + t * (k4 + t * k5)))
        t = t - f / slope
    heat = k1 + t * (k2 + t * (k3 + t * (k4 + t * k5)))
    g = gas / heat
    p = gas * t
    c = jnp.sqrt((1.0 + g) * p * inv)
    half_q = 0.5 * square * inv * inv
    half_g, half_t = 0.5 * g, 0.5 * t
    phi = []
    for i in range(NS):
        e = tab_ref[i, 6] + t * (
            tab_ref[i, 1]
            + t * (tab_ref[i, 7] + t * (tab_ref[i, 8] + t * (tab_ref[i, 9] + t * tab_ref[i, 10])))
        )
        phi.append(tab_ref[i, 0] * half_t - half_g * (e - half_q))
    half_inv = 0.5 * inv
    cell = [u[i] * inv for i in range(NS)]
    cell += [u[k] * half_inv for k in (NM, T1, T2)]
    cell += [u[SC] * inv, half_g, 0.5 * c] + phi + [p, rho]
    speed = [jnp.abs(u[k] * inv) + c for k in (NM, T1, T2)]
    return cell, speed


def flux_rows(u, half_v, p, rho, alpha):
    v = half_v + half_v
    plus, minus = [], []
    for k in range(NVAR):
        if k == EN:
            f = (u[k] + p) * v
        elif k == NM:
            f = u[k] * v + p
        else:
            f = u[k] * v
        a = alpha * u[k]
        plus.append(f + a)
        minus.append(f - a)
    a = alpha * rho
    plus.append(u[NM] + a)
    minus.append(u[NM] - a)
    return plus, minus


def weno(d0, d1, d2, d3):
    eps = 3.0 * EPSILON
    a1, a2 = d1 * d1, d2 * d2
    s0 = d0 * (d0 - 2.75 * d1) + (2.5 * a1 + eps)
    s2 = d3 * (d3 - 2.75 * d2) + (2.5 * a2 + eps)
    s1 = (a1 - 1.25 * (d1 * d2)) + (a2 + eps)
    r0, r1, r2 = 1.0 / s0, 1.0 / s1, 1.0 / s2
    w0, w1, w2 = r0 * r0, r1 * r1, 3.0 * (r2 * r2)
    c0, c1, c2 = d1 - d0, d2 - d1, d3 - d2
    x0 = w0 * (c1 - c0)
    number = (x0 + x0) + w2 * (c2 - c1)
    total = (w0 + w2) + 6.0 * w1
    return ((d1 + d2) + d2) - number / total


def face_row(cell, diff, base):
    low, high = cell
    mean = [low[n] + high[n] for n in range(CP)]
    y = mean[CY : CY + NS]
    vn, v1, v2 = mean[CU : CU + 3]
    z, g, c = mean[CZ], mean[CG], mean[CC]
    phi = mean[CPHI : CPHI + NS]
    half_over_c = 0.5 / c
    half_over_cc = 2.0 * half_over_c * half_over_c

    def split(d):
        dp = phi[0] * d[0]
        for i in range(1, NS):
            dp = dp + phi[i] * d[i]
        work = vn * d[NM] + v1 * d[T1] + v2 * d[T2]
        dp = dp + g * (d[EN] - work)
        total = d[NVAR]
        a = dp * half_over_cc
        b = (d[NM] - vn * total) * half_over_c
        return a, a - b, a + b, d[T1] - v1 * total, d[T2] - v2 * total, d[SC] - z * a

    parts = [split(d) for d in diff]

    def both(values):
        return weno(*values[:4]) - weno(*values[4:])

    slow, fast, shear1, shear2, scalar = [both([p[n] for p in parts]) for n in range(1, 6)]
    species = [both([d[i] - y[i] * p[0] for d, p in zip(diff, parts)]) for i in range(NS)]
    acoustic = slow + fast
    half_acoustic = 0.5 * acoustic
    pull = c * (fast - slow)
    total = species[0]
    for i in range(1, NS):
        total = total + species[i]
    carried = acoustic + total
    weight = c * c - 0.5 * functools.reduce(lambda s, i: s + y[i] * phi[i], range(1, NS), y[0] * phi[0])
    heat = functools.reduce(lambda s, i: s + species[i] * phi[i], range(1, NS), species[0] * phi[0])
    square = vn * vn + v1 * v1 + v2 * v2
    energy = (
        (weight * acoustic - heat) / g
        + square * carried
        + vn * pull
        + v1 * shear1
        + v2 * shear2
    )
    rows = [species[i] + y[i] * half_acoustic for i in range(NS)]
    rows += [vn * carried + pull, v1 * carried + shear1, v2 * carried + shear2, energy]
    rows += [z * half_acoustic + scalar]
    return [6.0 * base[k] + rows[k] for k in range(NVAR)]


def compute_kernel(
    u_ref, xl_ref, xh_ref, yl_ref, yh_ref, alpha_ref, nasa_ref, gas_ref, index_ref, kind_ref, out_ref,
    tab, uq, cq, ps, ms, dp, dm, fx, tmp,
):
    fill_table(nasa_ref, gas_ref, index_ref, tab)
    lane = lax.broadcasted_iota(jnp.int32, (8, 128), 1)
    sub = lax.broadcasted_iota(jnp.int32, (8, 128), 0)
    left = lane < 64

    for k in range(NVAR):
        cx, cy = ORDER[0][k], ORDER[1][k]
        for r in range(8):
            uq[3 + r, k] = u_ref[cx, 8 * r : 8 * r + 8, :]
            uq[ROWS + 3 + r, k] = u_ref[cy, pl.ds(r, 8, stride=8), :]
        for r in range(3):
            uq[r, k] = xl_ref[cx, 8 * r : 8 * r + 8, :]
            uq[11 + r, k] = xh_ref[cx, 8 * r : 8 * r + 8, :]
            uq[ROWS + r, k] = yl_ref[r, cy]
            uq[ROWS + 11 + r, k] = yh_ref[r, cy]
    zb = 2 * ROWS
    for pair in range(NVAR // 2):
        a, b = 2 * pair, 2 * pair + 1
        both = jnp.concatenate([u_ref[a], u_ref[b]], axis=0)
        turned = jnp.transpose(both)
        for t in range(8):
            lo, hi = turned[8 * t : 8 * t + 8], turned[64 + 8 * t : 72 + 8 * t]
            tmp[a, 8 * t : 8 * t + 8, :] = jnp.where(left, lo, pltpu.roll(hi, 64, 1))
            tmp[b, 8 * t : 8 * t + 8, :] = jnp.where(left, pltpu.roll(lo, 64, 1), hi)
    low_kind, high_kind = kind_ref[0, 0, 0], kind_ref[0, 0, 1]
    low_wall, high_wall = (low_kind == 1), (high_kind == 1)
    for k in range(NVAR):
        cz = ORDER[2][k]
        rows = [tmp[cz, pl.ds(l, 8, stride=8), :] for l in range(8)]
        for l in range(8):
            uq[zb + 3 + l, k] = rows[l]
        sign = -1.0 if k == NM else 1.0
        for n in range(3):
            inside = pltpu.roll(rows[7 - n], 1, 0)
            ghost = jnp.where(low_wall, sign * rows[n], rows[0])
            edge = jnp.where(left, ghost, pltpu.roll(inside, 64, 1))
            uq[zb + 2 - n, k] = jnp.where(sub == 0, edge, inside)
            inside = pltpu.roll(rows[n], 7, 0)
            ghost = jnp.where(high_wall, sign * rows[7 - n], rows[7])
            edge = jnp.where(left, pltpu.roll(inside, 64, 1), ghost)
            uq[zb + 11 + n, k] = jnp.where(sub == 7, edge, inside)

    @pl.loop(0, 3 * ROWS)
    def _(r):
        cell, _ = cell_row([uq[r, k] for k in range(NVAR)], tab)
        for n in range(NCELL):
            cq[r, n] = cell[n]

    @pl.loop(0, 3)
    def _(d):
        first = d * ROWS
        alpha = alpha_ref[0, d]

        @pl.loop(0, ROWS)
        def _(r):
            plus, minus = flux_rows(
                [uq[first + r, k] for k in range(NVAR)],
                cq[first + r, CU], cq[first + r, CP], cq[first + r, CRHO], alpha,
            )
            for k in range(NFLUX):
                ps[r, k] = plus[k]
                ms[r, k] = minus[k]

        @pl.loop(0, ROWS - 1)
        def _(r):
            for k in range(NFLUX):
                dp[r, k] = ps[r + 1, k] - ps[r, k]
                dm[r, k] = ms[r + 1, k] - ms[r, k]

        @pl.loop(0, FACES)
        def _(f):
            diff = [[dp[f + n, k] for k in range(NFLUX)] for n in (0, 1, 2, 3)]
            diff += [[dm[f + n, k] for k in range(NFLUX)] for n in (4, 3, 2, 1)]
            base = [ps[f + 2, k] + ms[f + 3, k] for k in range(NVAR)]
            cell = [[cq[first + f + n, k] for k in range(CP)] for n in (2, 3)]
            flux = face_row(cell, diff, base)
            for k in range(NVAR):
                fx[d * FACES + f, k] = flux[k]

    scale = (COURANT / 12.0) / (alpha_ref[0, 0] + alpha_ref[0, 1] + alpha_ref[0, 2])
    for k in range(NVAR):
        for r in range(8):
            tmp[ORDER[1][k], 8 * r : 8 * r + 8, :] = fx[FACES + r, k] - fx[FACES + r + 1, k]
    for k in range(NVAR):
        for r in range(8):
            rate = (fx[r, k] - fx[r + 1, k]) + tmp[k, pl.ds(r, 8, stride=8), :]
            out_ref[k, 8 * r : 8 * r + 8, :] = rate
    for k in range(NVAR):
        for r in range(8):
            tmp[ORDER[2][k], 8 * r : 8 * r + 8, :] = fx[2 * FACES + r, k] - fx[2 * FACES + r + 1, k]
    for pair in range(NVAR // 2):
        a, b = 2 * pair, 2 * pair + 1
        low, high = [], []
        for t in range(8):
            ra = tmp[a, pl.ds(t, 8, stride=8), :]
            rb = tmp[b, pl.ds(t, 8, stride=8), :]
            low.append(jnp.where(left, ra, pltpu.roll(rb, 64, 1)))
            high.append(jnp.where(left, pltpu.roll(ra, 64, 1), rb))
        back = jnp.transpose(jnp.concatenate(low + high, axis=0))
        out_ref[a] = scale * (out_ref[a] + back[:64])
        out_ref[b] = scale * (out_ref[b] + back[64:])


def compute(u, halos, alpha, nasa, gas, index, kind):
    vmem = pl.BlockSpec(memory_space=pltpu.VMEM)
    smem = pl.BlockSpec(memory_space=pltpu.SMEM)
    f32 = jnp.float32
    return pl.pallas_call(
        compute_kernel,
        out_shape=jax.ShapeDtypeStruct((NVAR, 64, 128), f32),
        in_specs=[vmem] * 5 + [smem] * 5,
        out_specs=vmem,
        scratch_shapes=[
            pltpu.SMEM((NS, 11), f32),
            pltpu.VMEM((3 * ROWS, NVAR, 8, 128), f32),
            pltpu.VMEM((3 * ROWS, NCELL, 8, 128), f32),
            pltpu.VMEM((ROWS, NFLUX, 8, 128), f32),
            pltpu.VMEM((ROWS, NFLUX, 8, 128), f32),
            pltpu.VMEM((ROWS, NFLUX, 8, 128), f32),
            pltpu.VMEM((ROWS, NFLUX, 8, 128), f32),
            pltpu.VMEM((3 * FACES, NVAR, 8, 128), f32),
            pltpu.VMEM((NVAR, 64, 128), f32),
        ],
    )(u, *halos, alpha, nasa, gas, index, kind)


MESH = pl.DeviceIdType.MESH


def exchange_kernel(
    u_ref, nasa_ref, gas_ref, index_ref, alpha_ref, xl_ref, xh_ref, yl_ref, yh_ref,
    tab, uy, mine, slots, halo_send, halo_recv, speed_send, speed_recv,
):
    gx, gy = lax.axis_index("gx"), lax.axis_index("gy")
    nx, ny = lax.axis_size("gx"), lax.axis_size("gy")
    z, y_low, plane, core = gx // 2, gx % 2, gy // 2, gy % 2
    me = (y_low * (ny // 2) + plane, z * 2 + core)
    size = (ny, nx)

    def member(stage, j):
        if stage == 0:
            return (2 * z + j // (ny // 2), 2 * (j % (ny // 2)) + core)
        return (2 * (j // 2) + y_low, 2 * plane + j % 2)

    others = [[(me[s] + n) % size[s] for n in range(1, size[s])] for s in (0, 1)]
    beside = [
        ((gx + 1) % nx, gy),
        ((gx + nx - 1) % nx, gy),
        (gx, (gy + 1) % ny),
        (gx, (gy + ny - 1) % ny),
    ]
    barrier = pltpu.get_barrier_semaphore()
    peers = beside + [member(s, j) for s in (0, 1) for j in others[s]]
    for peer in peers:
        pl.semaphore_signal(barrier, inc=1, device_id=peer, device_id_type=MESH)

    fill_table(nasa_ref, gas_ref, index_ref, tab)
    best = None
    for r in range(8):
        _, speed = cell_row([u_ref[k, 8 * r : 8 * r + 8, :] for k in range(NVAR)], tab)
        best = speed if best is None else [jnp.maximum(a, b) for a, b in zip(best, speed)]
    lane = lax.broadcasted_iota(jnp.int32, (1, 128), 1)
    row = jnp.zeros((1, 128), jnp.float32)
    for d in range(3):
        row = jnp.where(lane == d, jnp.max(best[d], keepdims=True), row)
    mine[0] = row
    for k in range(NVAR):
        for n, r in enumerate((0, 1, 2, 5, 6, 7)):
            uy[n, k] = u_ref[k, pl.ds(r, 8, stride=8), :]

    pl.semaphore_wait(barrier, len(peers))

    def speed_copy(stage, n, j, slot):
        return pltpu.make_async_remote_copy(
            src_ref=mine.at[stage],
            dst_ref=slots.at[stage, slot],
            send_sem=speed_send.at[stage, n],
            recv_sem=speed_recv.at[stage, slot],
            device_id=member(stage, j),
            device_id_type=MESH,
        )

    def gather(stage):
        for n, j in enumerate(others[stage]):
            speed_copy(stage, n, j, me[stage]).start()

    def reduce(stage):
        total = mine[stage]
        for n, j in enumerate(others[stage]):
            speed_copy(stage, n, j, j).wait_recv()
        for n, j in enumerate(others[stage]):
            total = jnp.maximum(total, slots[stage, j])
        return total

    gather(0)
    pieces = (
        (u_ref.at[:, 40:64, :], xl_ref),
        (u_ref.at[:, 0:24, :], xh_ref),
        (uy.at[3:6], yl_ref),
        (uy.at[0:3], yh_ref),
    )
    halos = []
    for n, (source, target) in enumerate(pieces):
        copy = pltpu.make_async_remote_copy(
            src_ref=source,
            dst_ref=target,
            send_sem=halo_send.at[n],
            recv_sem=halo_recv.at[n],
            device_id=beside[n],
            device_id_type=MESH,
        )
        copy.start()
        halos.append(copy)
    mine[1] = reduce(0)
    gather(1)
    alpha_ref[...] = reduce(1)
    for copy in halos:
        copy.wait()
    for stage in (0, 1):
        for n, j in enumerate(others[stage]):
            speed_copy(stage, n, j, me[stage]).wait_send()


def exchange(u, nasa, gas, index):
    vmem = pl.BlockSpec(memory_space=pltpu.VMEM)
    smem = pl.BlockSpec(memory_space=pltpu.SMEM)
    f32 = jnp.float32
    shape = jax.ShapeDtypeStruct
    return pl.pallas_call(
        exchange_kernel,
        out_shape=[
            shape((1, 128), f32),
            shape((NVAR, 24, 128), f32),
            shape((NVAR, 24, 128), f32),
            shape((3, NVAR, 8, 128), f32),
            shape((3, NVAR, 8, 128), f32),
        ],
        in_specs=[vmem] + [smem] * 3,
        out_specs=[vmem] * 5,
        scratch_shapes=[
            pltpu.SMEM((NS, 11), f32),
            pltpu.VMEM((6, NVAR, 8, 128), f32),
            pltpu.VMEM((2, 1, 128), f32),
            pltpu.VMEM((2, 16, 1, 128), f32),
            pltpu.SemaphoreType.DMA((4,)),
            pltpu.SemaphoreType.DMA((4,)),
            pltpu.SemaphoreType.DMA((2, 16)),
            pltpu.SemaphoreType.DMA((2, 16)),
        ],
        compiler_params=pltpu.CompilerParams(collective_id=0, has_side_effects=True),
    )(u, nasa, gas, index)


def solution(mesh):
    def shards(u, nasa, gas, index, kind):
        flat = u.reshape(NVAR, 64, 128)
        alpha, *halos = exchange(flat, nasa, gas, index)
        return compute(flat, halos, alpha, nasa, gas, index, kind).reshape(u.shape)

    whole = P(None, "gx", "gy", None)
    return jax.shard_map(
        shards, mesh=mesh, in_specs=(whole, P(), P(), P(), P("gx", "gy", None)), out_specs=whole, check_vma=False
    )
```

```python
import functools

import jax
import jax.numpy as jnp
from jax import lax
from jax.experimental import pallas as pl
from jax.experimental.pallas import tpu as pltpu
from jax.sharding import PartitionSpec as P

NS = 9
NVAR = 14
NEWTON = 2
EPSILON = 1e-06
COURANT = 0.8

ROWS = 14
FACES = 9
ORDER = (
    tuple(range(9)) + (9, 10, 11, 12, 13),
    tuple(range(9)) + (10, 9, 11, 12, 13),
    tuple(range(9)) + (11, 9, 10, 12, 13),
)
NM = 9
T1, T2, EN, SC = 10, 11, 12, 13
CY, CU, CZ, CG, CC, CPHI, CRHO, CF = 0, 9, 12, 13, 14, 15, 24, 25
NCELL = 39
FINV, FWEIGHT, FSQUARE = 24, 25, 26
NFACE = 27
MESH = pl.DeviceIdType.MESH


def fill_table(nasa_ref, gas_ref, index_ref, tab_ref):
    for i in range(NS):
        k = index_ref[i]
        r = gas_ref[k]
        a = [nasa_ref[n, k] for n in range(6)]
        tab_ref[i, 0] = r
        tab_ref[i, 1] = r * (a[0] - 1.0)
        tab_ref[i, 2] = r * a[1]
        tab_ref[i, 3] = r * a[2]
        tab_ref[i, 4] = r * a[3]
        tab_ref[i, 5] = r * a[4]
        tab_ref[i, 6] = r * a[5]
        tab_ref[i, 7] = r * a[1] * 0.5
        tab_ref[i, 8] = r * a[2] * (1.0 / 3.0)
        tab_ref[i, 9] = r * a[3] * 0.25
        tab_ref[i, 10] = r * a[4] * 0.2


def cell_row(u, tab_ref):
    rho = u[0]
    for i in range(1, NS):
        rho = rho + u[i]
    inv = 1.0 / rho
    square = u[NM] * u[NM] + u[T1] * u[T1] + u[T2] * u[T2]
    energy = u[EN] - 0.5 * square * inv
    moment = []
    for n in range(7):
        total = u[0] * tab_ref[0, n]
        for i in range(1, NS):
            total = total + u[i] * tab_ref[i, n]
        moment.append(total)
    gas, k1, k2, k3, k4, k5, k6 = moment
    l2, l3, l4, l5 = k2 * 0.5, k3 * (1.0 / 3.0), k4 * 0.25, k5 * 0.2
    base = k6 - energy
    t = 1.0
    for _ in range(NEWTON):
        f = base + t * (k1 + t * (l2 + t * (l3 + t * (l4 + t * l5))))
        slope = k1 + t * (k2 + t * (k3 + t * (k4 + t * k5)))
        t = t - f / slope
    heat = k1 + t * (k2 + t * (k3 + t * (k4 + t * k5)))
    g = gas / heat
    p = gas * t
    c = jnp.sqrt((1.0 + g) * p * inv)
    half_q = 0.5 * square * inv * inv
    half_g, half_t = 0.5 * g, 0.5 * t
    phi = []
    for i in range(NS):
        e = tab_ref[i, 6] + t * (
            tab_ref[i, 1]
            + t * (tab_ref[i, 7] + t * (tab_ref[i, 8] + t * (tab_ref[i, 9] + t * tab_ref[i, 10])))
        )
        phi.append(tab_ref[i, 0] * half_t - half_g * (e - half_q))
    half_inv = 0.5 * inv
    cell = [u[i] * inv for i in range(NS)]
    cell += [u[k] * half_inv for k in (NM, T1, T2)]
    cell += [u[SC] * inv, half_g, 0.5 * c] + phi + [rho]
    v = u[NM] * inv
    flux = [u[k] * v for k in range(NVAR)]
    flux[NM] = flux[NM] + p
    flux[EN] = (u[EN] + p) * v
    cell += flux
    speed = [jnp.abs(u[k] * inv) + c for k in (NM, T1, T2)]
    return cell, speed


def correction(d0, d1, d2, d3):
    a1, a2 = d1 * d1, d2 * d2
    eps = 3.0 * EPSILON
    k1, k2 = 0.609375 * a1 + eps, 0.609375 * a2 + eps
    y0, y1, y2 = d0 - 1.375 * d1, d1 - 0.625 * d2, d3 - 1.375 * d2
    r0, r1, r2 = 1.0 / (y0 * y0 + k1), 1.0 / (y1 * y1 + k2), 1.0 / (y2 * y2 + k2)
    w0, w1, w2 = r0 * r0, r1 * r1, 3.0 * (r2 * r2)
    c0, c1, c2 = d1 - d0, d2 - d1, d3 - d2
    x0 = w0 * (c1 - c0)
    number = (x0 + x0) + w2 * (c2 - c1)
    total = (w0 + w2) + 6.0 * w1
    return number / total


def dot(a, b):
    return functools.reduce(lambda s, n: s + a[n] * b[n], range(1, len(a)), a[0] * b[0])


def prepare(first, f, i, uq, cq, lf, lu, bf, bu, mean_ref):
    low, high = first + f + 2, first + f + 3
    mean = [cq[low, n] + cq[high, n] for n in range(CRHO)]
    y = mean[CY : CY + NS]
    vn, v1, v2 = mean[CU : CU + 3]
    z, g, c = mean[CZ], mean[CG], mean[CC]
    phi = mean[CPHI : CPHI + NS]
    for n in range(CRHO):
        mean_ref[i, n] = mean[n]
    mean_ref[i, FINV] = 1.0 / g
    mean_ref[i, FWEIGHT] = c * c - 0.5 * dot(y, phi)
    mean_ref[i, FSQUARE] = vn * vn + v1 * v1 + v2 * v2
    half_over_c = 0.5 / c
    half_over_cc = 2.0 * half_over_c * half_over_c

    def split(d, total):
        work = vn * d[NM] + v1 * d[T1] + v2 * d[T2]
        dp = dot(phi, d[:NS]) + g * (d[EN] - work)
        a = dp * half_over_cc
        b = (d[NM] - vn * total) * half_over_c
        parts = [d[k] - y[k] * a for k in range(NS)]
        return parts + [a - b, d[T1] - v1 * total, d[T2] - v2 * total, a + b, d[SC] - z * a]

    for n in range(5):
        here, there = first + f + n, first + f + n + 1
        du = [uq[there, k] - uq[here, k] for k in range(NVAR)]
        df = [cq[there, CF + k] - cq[here, CF + k] for k in range(NVAR)]
        parts = split(du, cq[there, CRHO] - cq[here, CRHO])
        for k in range(NVAR):
            lu[i, n, k] = parts[k]
        parts = split(df, du[NM])
        for k in range(NVAR):
            lf[i, n, k] = parts[k]
    for k in range(NVAR):
        f0, f1, f2, f3 = [cq[first + f + n, CF + k] for n in (1, 2, 3, 4)]
        bf[i, k] = 6.0 * (f1 + f2) + ((f1 - f0) - (f3 - f2))
    for k in range(NVAR):
        u0, u1, u2, u3 = [uq[first + f + n, k] for n in (1, 2, 3, 4)]
        bu[i, k] = (u3 - u0) - 3.0 * (u2 - u1)


def finish(alpha, i, lf, lu, bf, bu, mean_ref, fx):
    def wave(k):
        l = [lf[i, n, k] for n in range(5)]
        a = [alpha * lu[i, n, k] for n in range(5)]
        plus = correction(*[l[n] + a[n] for n in (0, 1, 2, 3)])
        minus = correction(*[l[n] - a[n] for n in (4, 3, 2, 1)])
        return minus - plus

    species = [wave(k) for k in range(NS)]
    slow, shear1, shear2, fast, scalar = [wave(k) for k in range(NS, NVAR)]
    mean = [mean_ref[i, n] for n in range(NFACE)]
    y, phi = mean[CY : CY + NS], mean[CPHI : CPHI + NS]
    vn, v1, v2 = mean[CU : CU + 3]
    acoustic = slow + fast
    half_acoustic = 0.5 * acoustic
    pull = mean[CC] * (fast - slow)
    carried = functools.reduce(lambda s, n: s + n, species, acoustic)
    energy = (
        (mean[FWEIGHT] * acoustic - dot(species, phi)) * mean[FINV]
        + mean[FSQUARE] * carried
        + vn * pull
        + v1 * shear1
        + v2 * shear2
    )
    rows = [species[k] + y[k] * half_acoustic for k in range(NS)]
    rows += [vn * carried + pull, v1 * carried + shear1, v2 * carried + shear2, energy]
    rows += [mean[CZ] * half_acoustic + scalar]
    for k in range(NVAR):
        fx[i, k] = (bf[i, k] + alpha * bu[i, k]) + rows[k]


def kernel(
    u_ref, nasa_ref, gas_ref, index_ref, kind_ref, out_ref,
    tab, uq, cq, lf, lu, bf, bu, mean_ref, fx, tmp, alphas,
    mine, slots, halo_send, halo_recv, speed_send, speed_recv,
):
    gx, gy = lax.axis_index("gx"), lax.axis_index("gy")
    nx, ny = lax.axis_size("gx"), lax.axis_size("gy")
    z, y_low, plane, core = gx // 2, gx % 2, gy // 2, gy % 2
    me = (y_low * (ny // 2) + plane, z * 2 + core)
    size = (ny, nx)

    def member(stage, j):
        if stage == 0:
            return (2 * z + j // (ny // 2), 2 * (j % (ny // 2)) + core)
        return (2 * (j // 2) + y_low, 2 * plane + j % 2)

    others = [[(me[s] + n) % size[s] for n in range(1, size[s])] for s in (0, 1)]
    beside = [
        ((gx + 1) % nx, gy),
        ((gx + nx - 1) % nx, gy),
        (gx, (gy + 1) % ny),
        (gx, (gy + ny - 1) % ny),
    ]
    barrier = pltpu.get_barrier_semaphore()
    peers = beside + [member(s, j) for s in (0, 1) for j in others[s]]
    for peer in peers:
        pl.semaphore_signal(barrier, inc=1, device_id=peer, device_id_type=MESH)

    fill_table(nasa_ref, gas_ref, index_ref, tab)
    lane = lax.broadcasted_iota(jnp.int32, (8, 128), 1)
    sub = lax.broadcasted_iota(jnp.int32, (8, 128), 0)
    left = lane < 64
    yb, zb = ROWS, 2 * ROWS

    for k in range(NVAR):
        cx, cy = ORDER[0][k], ORDER[1][k]
        for r in range(8):
            uq[3 + r, k] = u_ref[cx, 8 * r : 8 * r + 8, :]
            uq[yb + 3 + r, k] = u_ref[cy, pl.ds(r, 8, stride=8), :]

    def cells(r):
        cell, speed = cell_row([uq[r, k] for k in range(NVAR)], tab)
        for n in range(NCELL):
            cq[r, n] = cell[n]
        return speed

    zero = jnp.zeros((8, 128), jnp.float32)
    best = lax.fori_loop(
        3, 11, lambda r, best: tuple(jnp.maximum(a, b) for a, b in zip(best, cells(r))), (zero, zero, zero)
    )
    row = jnp.zeros((1, 128), jnp.float32)
    for d in range(3):
        row = jnp.where(lane[:1] == d, jnp.max(best[d], keepdims=True), row)
    mine[0] = row

    pl.semaphore_wait(barrier, len(peers))

    def speed_copy(stage, n, j, slot):
        return pltpu.make_async_remote_copy(
            src_ref=mine.at[stage],
            dst_ref=slots.at[stage, slot],
            send_sem=speed_send.at[stage, n],
            recv_sem=speed_recv.at[stage, slot],
            device_id=member(stage, j),
            device_id_type=MESH,
        )

    def gather(stage):
        for n, j in enumerate(others[stage]):
            speed_copy(stage, n, j, me[stage]).start()

    def reduce(stage):
        total = mine[stage]
        for n, j in enumerate(others[stage]):
            speed_copy(stage, n, j, j).wait_recv()
        for n, j in enumerate(others[stage]):
            total = jnp.maximum(total, slots[stage, j])
        return total

    gather(0)
    pieces = ((8, 0), (3, 11), (yb + 8, yb), (yb + 3, yb + 11))
    halos = [
        pltpu.make_async_remote_copy(
            src_ref=uq.at[source : source + 3],
            dst_ref=uq.at[target : target + 3],
            send_sem=halo_send.at[n],
            recv_sem=halo_recv.at[n],
            device_id=beside[n],
            device_id_type=MESH,
        )
        for n, (source, target) in enumerate(pieces)
    ]
    for copy in halos:
        copy.start()

    for pair in range(NVAR // 2):
        a, b = 2 * pair, 2 * pair + 1
        turned = jnp.transpose(jnp.concatenate([u_ref[a], u_ref[b]], axis=0))
        for t in range(8):
            lo, hi = turned[8 * t : 8 * t + 8], turned[64 + 8 * t : 72 + 8 * t]
            tmp[a, 8 * t : 8 * t + 8, :] = jnp.where(left, lo, pltpu.roll(hi, 64, 1))
            tmp[b, 8 * t : 8 * t + 8, :] = jnp.where(left, pltpu.roll(lo, 64, 1), hi)
    low_wall, high_wall = kind_ref[0, 0, 0] == 1, kind_ref[0, 0, 1] == 1
    for k in range(NVAR):
        cz = ORDER[2][k]
        rows = [tmp[cz, pl.ds(l, 8, stride=8), :] for l in range(8)]
        for l in range(8):
            uq[zb + 3 + l, k] = rows[l]
        sign = -1.0 if k == NM else 1.0
        for n in range(3):
            inside = pltpu.roll(rows[7 - n], 1, 0)
            ghost = jnp.where(low_wall, sign * rows[n], rows[0])
            edge = jnp.where(left, ghost, pltpu.roll(inside, 64, 1))
            uq[zb + 2 - n, k] = jnp.where(sub == 0, edge, inside)
            inside = pltpu.roll(rows[n], 7, 0)
            ghost = jnp.where(high_wall, sign * rows[7 - n], rows[7])
            edge = jnp.where(left, pltpu.roll(inside, 64, 1), ghost)
            uq[zb + 11 + n, k] = jnp.where(sub == 7, edge, inside)

    def before(first, f, i):
        prepare(first, f, i, uq, cq, lf, lu, bf, bu, mean_ref)

    @pl.loop(zb, zb + ROWS)
    def _(r):
        cells(r)

    @pl.loop(yb + 3, yb + 11)
    def _(r):
        cells(r)

    @pl.loop(0, FACES)
    def _(f):
        before(zb, f, 2 * FACES + f)

    @pl.loop(3, 6)
    def _(f):
        before(yb, f, FACES + f)

    mine[1] = reduce(0)
    gather(1)

    halos[0].wait_recv()
    halos[1].wait_recv()

    @pl.loop(0, 6)
    def _(n):
        cells(n + 8 * (n // 3))

    @pl.loop(0, FACES)
    def _(f):
        before(0, f, f)

    speeds = reduce(1)
    total = None
    for d in range(3):
        alpha = jnp.max(jnp.where(lane[:1] == d, speeds, 0.0), keepdims=True)
        alphas[d] = jnp.broadcast_to(alpha, (8, 128))
        total = alphas[d] if total is None else total + alphas[d]
    scale = (COURANT / 12.0) / total

    def after(d, i):
        finish(alphas[d], i, lf, lu, bf, bu, mean_ref, fx)

    @pl.loop(0, 2 * FACES)
    def _(n):
        half = n // FACES
        after(2 * half, n + FACES * half)

    halos[2].wait_recv()
    halos[3].wait_recv()

    @pl.loop(0, 6)
    def _(n):
        cells(yb + n + 8 * (n // 3))

    @pl.loop(0, 6)
    def _(n):
        f = n + 3 * (n // 3)
        before(yb, f, FACES + f)

    @pl.loop(FACES, 2 * FACES)
    def _(i):
        after(1, i)

    for k in range(NVAR):
        for r in range(8):
            tmp[ORDER[1][k], 8 * r : 8 * r + 8, :] = fx[FACES + r, k] - fx[FACES + r + 1, k]
    for k in range(NVAR):
        for r in range(8):
            rate = (fx[r, k] - fx[r + 1, k]) + tmp[k, pl.ds(r, 8, stride=8), :]
            out_ref[k, 8 * r : 8 * r + 8, :] = rate
    for k in range(NVAR):
        for r in range(8):
            tmp[ORDER[2][k], 8 * r : 8 * r + 8, :] = fx[2 * FACES + r, k] - fx[2 * FACES + r + 1, k]
    for pair in range(NVAR // 2):
        a, b = 2 * pair, 2 * pair + 1
        low, high = [], []
        for t in range(8):
            ra = tmp[a, pl.ds(t, 8, stride=8), :]
            rb = tmp[b, pl.ds(t, 8, stride=8), :]
            low.append(jnp.where(left, ra, pltpu.roll(rb, 64, 1)))
            high.append(jnp.where(left, pltpu.roll(ra, 64, 1), rb))
        back = jnp.transpose(jnp.concatenate(low + high, axis=0))
        for r in range(8):
            here = slice(8 * r, 8 * r + 8)
            out_ref[a, here] = scale * (out_ref[a, here] + back[8 * r : 8 * r + 8])
            out_ref[b, here] = scale * (out_ref[b, here] + back[64 + 8 * r : 72 + 8 * r])

    for copy in halos:
        copy.wait_send()
    for stage in (0, 1):
        for n, j in enumerate(others[stage]):
            speed_copy(stage, n, j, me[stage]).wait_send()


def solution(mesh):
    def shards(u, nasa, gas, index, kind):
        vmem = pl.BlockSpec(memory_space=pltpu.VMEM)
        smem = pl.BlockSpec(memory_space=pltpu.SMEM)
        f32 = jnp.float32

        def rows(*lead):
            return pltpu.VMEM(lead + (8, 128), f32)

        out = pl.pallas_call(
            kernel,
            out_shape=jax.ShapeDtypeStruct((NVAR, 64, 128), f32),
            in_specs=[vmem] + [smem] * 4,
            out_specs=vmem,
            scratch_shapes=[
                pltpu.SMEM((NS, 11), f32),
                rows(3 * ROWS, NVAR),
                rows(3 * ROWS, NCELL),
                rows(3 * FACES, 5, NVAR),
                rows(3 * FACES, 5, NVAR),
                rows(3 * FACES, NVAR),
                rows(3 * FACES, NVAR),
                rows(3 * FACES, NFACE),
                rows(3 * FACES, NVAR),
                pltpu.VMEM((NVAR, 64, 128), f32),
                rows(3),
                pltpu.VMEM((2, 1, 128), f32),
                pltpu.VMEM((2, 16, 1, 128), f32),
                pltpu.SemaphoreType.DMA((4,)),
                pltpu.SemaphoreType.DMA((4,)),
                pltpu.SemaphoreType.DMA((2, 16)),
                pltpu.SemaphoreType.DMA((2, 16)),
            ],
            compiler_params=pltpu.CompilerParams(
                collective_id=0, has_side_effects=True, vmem_limit_bytes=56 * 1024 * 1024
            ),
        )(u.reshape(NVAR, 64, 128), nasa.T, gas, index, kind)
        return out.reshape(u.shape)

    whole = P(None, "gx", "gy", None)
    return jax.shard_map(
        shards, mesh=mesh, in_specs=(whole, P(), P(), P(), P("gx", "gy", None)), out_specs=whole, check_vma=False
    )
```

```python
import functools

import jax
import jax.numpy as jnp
from jax import lax
from jax.experimental import pallas as pl
from jax.experimental.pallas import tpu as pltpu
from jax.sharding import PartitionSpec as P

NS = 9
NVAR = 14
NEWTON = 2
EPSILON = 1e-06
COURANT = 0.8

ROWS = 14
FACES = 9
ORDER = (
    tuple(range(9)) + (9, 10, 11, 12, 13),
    tuple(range(9)) + (10, 9, 11, 12, 13),
    tuple(range(9)) + (11, 9, 10, 12, 13),
)
NM = 9
T1, T2, EN, SC = 10, 11, 12, 13
CY, CU, CZ, CG, CC, CPHI, CRHO, CF = 0, 9, 12, 13, 14, 15, 24, 25
NCELL = 39
FINV, FWEIGHT, FSQUARE = 24, 25, 26
NFACE = 27
MESH = pl.DeviceIdType.MESH


def fill_table(nasa_ref, gas_ref, index_ref, tab_ref):
    for i in range(NS):
        k = index_ref[i]
        r = gas_ref[k]
        a = [nasa_ref[n, k] for n in range(6)]
        tab_ref[i, 0] = r
        tab_ref[i, 1] = r * (a[0] - 1.0)
        tab_ref[i, 2] = r * a[1]
        tab_ref[i, 3] = r * a[2]
        tab_ref[i, 4] = r * a[3]
        tab_ref[i, 5] = r * a[4]
        tab_ref[i, 6] = r * a[5]
        tab_ref[i, 7] = r * a[1] * 0.5
        tab_ref[i, 8] = r * a[2] * (1.0 / 3.0)
        tab_ref[i, 9] = r * a[3] * 0.25
        tab_ref[i, 10] = r * a[4] * 0.2


def cell_row(u, tab_ref):
    rho = u[0]
    for i in range(1, NS):
        rho = rho + u[i]
    inv = 1.0 / rho
    square = u[NM] * u[NM] + u[T1] * u[T1] + u[T2] * u[T2]
    energy = u[EN] - 0.5 * square * inv
    moment = []
    for n in range(7):
        total = u[0] * tab_ref[0, n]
        for i in range(1, NS):
            total = total + u[i] * tab_ref[i, n]
        moment.append(total)
    gas, k1, k2, k3, k4, k5, k6 = moment
    l2, l3, l4, l5 = k2 * 0.5, k3 * (1.0 / 3.0), k4 * 0.25, k5 * 0.2
    base = k6 - energy
    t = 1.0
    for _ in range(NEWTON):
        f = base + t * (k1 + t * (l2 + t * (l3 + t * (l4 + t * l5))))
        slope = k1 + t * (k2 + t * (k3 + t * (k4 + t * k5)))
        t = t - f / slope
    heat = k1 + t * (k2 + t * (k3 + t * (k4 + t * k5)))
    g = gas / heat
    p = gas * t
    c = jnp.sqrt((1.0 + g) * p * inv)
    half_q = 0.5 * square * inv * inv
    half_g, half_t = 0.5 * g, 0.5 * t
    phi = []
    for i in range(NS):
        e = tab_ref[i, 6] + t * (
            tab_ref[i, 1]
            + t * (tab_ref[i, 7] + t * (tab_ref[i, 8] + t * (tab_ref[i, 9] + t * tab_ref[i, 10])))
        )
        phi.append(tab_ref[i, 0] * half_t - half_g * (e - half_q))
    half_inv = 0.5 * inv
    cell = [u[i] * inv for i in range(NS)]
    cell += [u[k] * half_inv for k in (NM, T1, T2)]
    cell += [u[SC] * inv, half_g, 0.5 * c] + phi + [rho]
    v = u[NM] * inv
    flux = [u[k] * v for k in range(NVAR)]
    flux[NM] = flux[NM] + p
    flux[EN] = (u[EN] + p) * v
    cell += flux
    speed = [jnp.abs(u[k] * inv) + c for k in (NM, T1, T2)]
    return cell, speed


def correction(d0, d1, d2, d3):
    a1, a2 = d1 * d1, d2 * d2
    eps = 3.0 * EPSILON
    k1, k2 = 0.609375 * a1 + eps, 0.609375 * a2 + eps
    y0, y1, y2 = d0 - 1.375 * d1, d1 - 0.625 * d2, d3 - 1.375 * d2
    r0, r1, r2 = 1.0 / (y0 * y0 + k1), 1.0 / (y1 * y1 + k2), 1.0 / (y2 * y2 + k2)
    w0, w1, w2 = r0 * r0, r1 * r1, 3.0 * (r2 * r2)
    c0, c1, c2 = d1 - d0, d2 - d1, d3 - d2
    x0 = w0 * (c1 - c0)
    number = (x0 + x0) + w2 * (c2 - c1)
    total = (w0 + w2) + 6.0 * w1
    return number / total


def dot(a, b):
    return functools.reduce(lambda s, n: s + a[n] * b[n], range(1, len(a)), a[0] * b[0])


def prepare(first, f, i, uq, cq, lf, lu, bf, bu, mean_ref):
    low, high = first + f + 2, first + f + 3
    mean = [cq[low, n] + cq[high, n] for n in range(CRHO)]
    y = mean[CY : CY + NS]
    vn, v1, v2 = mean[CU : CU + 3]
    z, g, c = mean[CZ], mean[CG], mean[CC]
    phi = mean[CPHI : CPHI + NS]
    for n in range(CRHO):
        mean_ref[i, n] = mean[n]
    mean_ref[i, FINV] = 1.0 / g
    mean_ref[i, FWEIGHT] = c * c - 0.5 * dot(y, phi)
    mean_ref[i, FSQUARE] = vn * vn + v1 * v1 + v2 * v2
    half_over_c = 0.5 / c
    half_over_cc = 2.0 * half_over_c * half_over_c

    def split(d, total):
        work = vn * d[NM] + v1 * d[T1] + v2 * d[T2]
        dp = dot(phi, d[:NS]) + g * (d[EN] - work)
        a = dp * half_over_cc
        b = (d[NM] - vn * total) * half_over_c
        parts = [d[k] - y[k] * a for k in range(NS)]
        return parts + [a - b, d[T1] - v1 * total, d[T2] - v2 * total, a + b, d[SC] - z * a]

    for n in range(5):
        here, there = first + f + n, first + f + n + 1
        du = [uq[there, k] - uq[here, k] for k in range(NVAR)]
        df = [cq[there, CF + k] - cq[here, CF + k] for k in range(NVAR)]
        parts = split(du, cq[there, CRHO] - cq[here, CRHO])
        for k in range(NVAR):
            lu[i, n, k] = parts[k]
        parts = split(df, du[NM])
        for k in range(NVAR):
            lf[i, n, k] = parts[k]
    for k in range(NVAR):
        f0, f1, f2, f3 = [cq[first + f + n, CF + k] for n in (1, 2, 3, 4)]
        bf[i, k] = 7.0 * (f1 + f2) - (f0 + f3)
    for k in range(NVAR):
        u0, u1, u2, u3 = [uq[first + f + n, k] for n in (1, 2, 3, 4)]
        bu[i, k] = (u3 - u0) - 3.0 * (u2 - u1)


def finish(alpha, i, lf, lu, bf, bu, mean_ref, fx):
    def wave(k):
        l = [lf[i, n, k] for n in range(5)]
        a = [alpha * lu[i, n, k] for n in range(5)]
        plus = correction(*[l[n] + a[n] for n in (0, 1, 2, 3)])
        minus = correction(*[l[n] - a[n] for n in (4, 3, 2, 1)])
        return minus - plus

    species = [wave(k) for k in range(NS)]
    slow, shear1, shear2, fast, scalar = [wave(k) for k in range(NS, NVAR)]
    mean = [mean_ref[i, n] for n in range(NFACE)]
    y, phi = mean[CY : CY + NS], mean[CPHI : CPHI + NS]
    vn, v1, v2 = mean[CU : CU + 3]
    acoustic = slow + fast
    half_acoustic = 0.5 * acoustic
    pull = mean[CC] * (fast - slow)
    carried = functools.reduce(lambda s, n: s + n, species, acoustic)
    energy = (
        (mean[FWEIGHT] * acoustic - dot(species, phi)) * mean[FINV]
        + mean[FSQUARE] * carried
        + vn * pull
        + v1 * shear1
        + v2 * shear2
    )
    rows = [species[k] + y[k] * half_acoustic for k in range(NS)]
    rows += [vn * carried + pull, v1 * carried + shear1, v2 * carried + shear2, energy]
    rows += [mean[CZ] * half_acoustic + scalar]
    for k in range(NVAR):
        fx[i, k] = (bf[i, k] + alpha * bu[i, k]) + rows[k]


def kernel(
    u_hbm, nasa_ref, gas_ref, index_ref, kind_ref, out_ref,
    u_ref, u_sem, tab, uq, cq, lf, lu, bf, bu, mean_ref, fx, tmp, alphas,
    mine, slots, halo_send, halo_recv, speed_send, speed_recv,
):
    gx, gy = lax.axis_index("gx"), lax.axis_index("gy")
    nx, ny = lax.axis_size("gx"), lax.axis_size("gy")
    z, y_low, plane, core = gx // 2, gx % 2, gy // 2, gy % 2
    nz, n_plane = nx // 2, ny // 2
    x, y_high = plane // 2, plane % 2
    steps = (
        sorted(
            ((dx, high, low) for dx in range(n_plane // 2) for high in (0, 1) for low in (0, 1)),
            key=lambda d: -min(d[0], n_plane // 2 - d[0]) - (0, 1, 2, 1)[2 * d[1] + d[2]],
        )[:-1],
        sorted(((dz, other) for dz in range(nz) for other in (0, 1)), key=lambda d: -min(d[0], nz - d[0]) - 0.1 * d[1])[:-1],
    )

    def member(stage, step, sign):
        if stage == 0:
            dx, high, low = step
            to_low, to_high = (y_low + low) % 2, (y_high + high) % 2
            to_x = (x + sign * dx + n_plane // 2) % (n_plane // 2)
            return (2 * z + to_low, 4 * to_x + 2 * to_high + core), 4 * to_x + 2 * to_high + to_low
        dz, other = step
        to_z, to_core = (z + sign * dz + nz) % nz, (core + other) % 2
        return (2 * to_z + y_low, 2 * plane + to_core), 2 * to_z + to_core

    me = (4 * x + 2 * y_high + y_low, 2 * z + core)
    beside = [
        ((gx + nx - 1 + 2 * y_low) % nx, gy),
        (gx + 1 - 2 * y_low, gy),
        (gx, (gy + 1) % ny),
        (gx, (gy + ny - 1) % ny),
    ]
    load = pltpu.make_async_copy(u_hbm, u_ref, u_sem)
    load.start()
    barrier = pltpu.get_barrier_semaphore()
    peers = [member(s, step, 1)[0] for s in (0, 1) for step in steps[s]] + beside
    for peer in peers:
        pl.semaphore_signal(barrier, inc=1, device_id=peer, device_id_type=MESH)

    fill_table(nasa_ref, gas_ref, index_ref, tab)
    lane = lax.broadcasted_iota(jnp.int32, (8, 128), 1)
    sub = lax.broadcasted_iota(jnp.int32, (8, 128), 0)
    left = lane < 64
    yb, zb = ROWS, 2 * ROWS

    load.wait()
    for k in range(NVAR):
        for r in range(8):
            uq[3 + r, k] = u_ref[ORDER[0][k], 8 * r : 8 * r + 8, :]

    def cells(r):
        cell, speed = cell_row([uq[r, k] for k in range(NVAR)], tab)
        for n in range(NCELL):
            cq[r, n] = cell[n]
        return speed

    zero = jnp.zeros((8, 128), jnp.float32)
    best = lax.fori_loop(
        3, 11, lambda r, best: tuple(jnp.maximum(a, b) for a, b in zip(best, cells(r))), (zero, zero, zero)
    )
    row = jnp.zeros((1, 128), jnp.float32)
    for d in range(3):
        row = jnp.where(lane[:1] == d, jnp.max(best[d], keepdims=True), row)
    mine[0] = row

    for pair in range(NVAR // 2):
        a, b = 2 * pair, 2 * pair + 1
        turned = jnp.transpose(jnp.concatenate([u_ref[a], u_ref[b]], axis=0))
        for t in range(8):
            lo, hi = turned[8 * t : 8 * t + 8], turned[64 + 8 * t : 72 + 8 * t]
            tmp[a, 8 * t : 8 * t + 8, :] = jnp.where(left, lo, pltpu.roll(hi, 64, 1))
            tmp[b, 8 * t : 8 * t + 8, :] = jnp.where(left, pltpu.roll(lo, 64, 1), hi)
    low_wall, high_wall = kind_ref[0, 0, 0] == 1, kind_ref[0, 0, 1] == 1
    for k in range(NVAR):
        cz = ORDER[2][k]
        rows = [tmp[cz, pl.ds(l, 8, stride=8), :] for l in range(8)]
        for l in range(8):
            uq[zb + 3 + l, k] = rows[l]
        sign = -1.0 if k == NM else 1.0
        for n in range(3):
            inside = pltpu.roll(rows[7 - n], 1, 0)
            ghost = jnp.where(low_wall, sign * rows[n], rows[0])
            edge = jnp.where(left, ghost, pltpu.roll(inside, 64, 1))
            uq[zb + 2 - n, k] = jnp.where(sub == 0, edge, inside)
            inside = pltpu.roll(rows[n], 7, 0)
            ghost = jnp.where(high_wall, sign * rows[7 - n], rows[7])
            edge = jnp.where(left, pltpu.roll(inside, 64, 1), ghost)
            uq[zb + 11 + n, k] = jnp.where(sub == 7, edge, inside)

    for k in range(NVAR):
        for r in range(8):
            uq[yb + 3 + r, k] = u_ref[ORDER[1][k], pl.ds(r, 8, stride=8), :]

    pl.semaphore_wait(barrier, len(peers))

    def speed_copy(stage, n, slot):
        return pltpu.make_async_remote_copy(
            src_ref=mine.at[stage],
            dst_ref=slots.at[stage, slot],
            send_sem=speed_send.at[stage, n],
            recv_sem=speed_recv.at[stage, slot],
            device_id=member(stage, steps[stage][n], 1)[0],
            device_id_type=MESH,
        )

    def gather(stage):
        for n in range(len(steps[stage])):
            speed_copy(stage, n, me[stage]).start()

    def reduce(stage):
        total = mine[stage]
        places = [member(stage, step, -1)[1] for step in steps[stage]]
        for n, slot in enumerate(places):
            speed_copy(stage, n, slot).wait_recv()
        for slot in places:
            total = jnp.maximum(total, slots[stage, slot])
        return total

    gather(0)
    pieces = (
        (3 + 5 * y_low, 11 - 11 * y_low),
        (8 - 5 * y_low, 11 * y_low),
        (yb + 8, yb),
        (yb + 3, yb + 11),
    )
    halos = [
        pltpu.make_async_remote_copy(
            src_ref=uq.at[pl.ds(source, 3)],
            dst_ref=uq.at[pl.ds(target, 3)],
            send_sem=halo_send.at[n],
            recv_sem=halo_recv.at[n],
            device_id=beside[n],
            device_id_type=MESH,
        )
        for n, (source, target) in enumerate(pieces)
    ]
    halos[0].start()

    def before(first, f, i):
        prepare(first, f, i, uq, cq, lf, lu, bf, bu, mean_ref)

    @pl.loop(zb, zb + ROWS)
    def _(r):
        cells(r)

    @pl.loop(yb + 3, yb + 11)
    def _(r):
        cells(r)

    halos[1].start()
    @pl.loop(0, FACES)
    def _(f):
        before(zb, f, 2 * FACES + f)

    mine[1] = reduce(0)
    gather(1)
    halos[2].start()
    halos[3].start()

    @pl.loop(0, 6)
    def _(n):
        d = n // 3
        f = 3 + n - 3 * d
        before(ROWS * d, f, FACES * d + f)

    speeds = reduce(1)
    total = None
    for d in range(3):
        alpha = jnp.max(jnp.where(lane[:1] == d, speeds, 0.0), keepdims=True)
        alphas[d] = jnp.broadcast_to(alpha, (8, 128))
        total = alphas[d] if total is None else total + alphas[d]
    scale = (COURANT / 12.0) / total

    def after(d, i):
        finish(alphas[d], i, lf, lu, bf, bu, mean_ref, fx)

    @pl.loop(0, FACES + 6)
    def _(n):
        half = n // FACES
        m = n - FACES * half
        d = 2 * (1 - half) + half * (m // 3)
        after(d, FACES * d + (1 - half) * m + half * (3 + m - 3 * (m // 3)))

    halos[0].wait_recv()
    halos[1].wait_recv()

    @pl.loop(0, 6)
    def _(n):
        cells(n + 8 * (n // 3))

    @pl.loop(0, 6)
    def _(n):
        f = n + 3 * (n // 3)
        before(0, f, f)

    @pl.loop(0, 6)
    def _(n):
        after(0, n + 3 * (n // 3))

    halos[2].wait_recv()
    halos[3].wait_recv()

    @pl.loop(0, 6)
    def _(n):
        cells(yb + n + 8 * (n // 3))

    @pl.loop(0, 6)
    def _(n):
        f = n + 3 * (n // 3)
        before(yb, f, FACES + f)

    @pl.loop(0, 6)
    def _(n):
        after(1, FACES + n + 3 * (n // 3))

    for k in range(NVAR):
        for r in range(8):
            tmp[ORDER[1][k], 8 * r : 8 * r + 8, :] = fx[FACES + r, k] - fx[FACES + r + 1, k]
    for k in range(NVAR):
        for r in range(8):
            rate = (fx[r, k] - fx[r + 1, k]) + tmp[k, pl.ds(r, 8, stride=8), :]
            out_ref[k, 8 * r : 8 * r + 8, :] = rate
    for k in range(NVAR):
        for r in range(8):
            tmp[ORDER[2][k], 8 * r : 8 * r + 8, :] = fx[2 * FACES + r, k] - fx[2 * FACES + r + 1, k]
    for pair in range(NVAR // 2):
        a, b = 2 * pair, 2 * pair + 1
        low, high = [], []
        for t in range(8):
            ra = tmp[a, pl.ds(t, 8, stride=8), :]
            rb = tmp[b, pl.ds(t, 8, stride=8), :]
            low.append(jnp.where(left, ra, pltpu.roll(rb, 64, 1)))
            high.append(jnp.where(left, pltpu.roll(ra, 64, 1), rb))
        back = jnp.transpose(jnp.concatenate(low + high, axis=0))
        for r in range(8):
            here = slice(8 * r, 8 * r + 8)
            out_ref[a, here] = scale * (out_ref[a, here] + back[8 * r : 8 * r + 8])
            out_ref[b, here] = scale * (out_ref[b, here] + back[64 + 8 * r : 72 + 8 * r])

    for copy in halos:
        copy.wait_send()
    for stage in (0, 1):
        for n in range(len(steps[stage])):
            speed_copy(stage, n, me[stage]).wait_send()


def solution(mesh):
    def shards(u, nasa, gas, index, kind):
        vmem = pl.BlockSpec(memory_space=pltpu.VMEM)
        smem = pl.BlockSpec(memory_space=pltpu.SMEM)
        f32 = jnp.float32

        def rows(*lead):
            return pltpu.VMEM(lead + (8, 128), f32)

        out = pl.pallas_call(
            kernel,
            out_shape=jax.ShapeDtypeStruct((NVAR, 64, 128), f32),
            in_specs=[pl.BlockSpec(memory_space=pl.ANY)] + [smem] * 4,
            out_specs=vmem,
            scratch_shapes=[
                pltpu.VMEM((NVAR, 64, 128), f32),
                pltpu.SemaphoreType.DMA,
                pltpu.SMEM((NS, 11), f32),
                rows(3 * ROWS, NVAR),
                rows(3 * ROWS, NCELL),
                rows(3 * FACES, 5, NVAR),
                rows(3 * FACES, 5, NVAR),
                rows(3 * FACES, NVAR),
                rows(3 * FACES, NVAR),
                rows(3 * FACES, NFACE),
                rows(3 * FACES, NVAR),
                pltpu.VMEM((NVAR, 64, 128), f32),
                rows(3),
                pltpu.VMEM((2, 1, 128), f32),
                pltpu.VMEM((2, 16, 1, 128), f32),
                pltpu.SemaphoreType.DMA((4,)),
                pltpu.SemaphoreType.DMA((4,)),
                pltpu.SemaphoreType.DMA((2, 16)),
                pltpu.SemaphoreType.DMA((2, 16)),
            ],
            compiler_params=pltpu.CompilerParams(
                collective_id=0, has_side_effects=True, vmem_limit_bytes=36 * 1024 * 1024
            ),
        )(*[pltpu.with_memory_space_constraint(a, pltpu.HBM) for a in (u.reshape(NVAR, 64, 128), nasa.T, gas, index, kind)])
        return out.reshape(u.shape)

    whole = P(None, "gx", "gy", None)
    return jax.shard_map(
        shards, mesh=mesh, in_specs=(whole, P(), P(), P(), P("gx", "gy", None)), out_specs=whole, check_vma=False
    )
```

```python
import functools

import jax
import jax.numpy as jnp
from jax import lax
from jax.experimental import pallas as pl
from jax.experimental.pallas import tpu as pltpu
from jax.sharding import PartitionSpec as P

NS = 9
NVAR = 14
NEWTON = 2
EPSILON = 1e-06
COURANT = 0.8

ROWS = 14
FACES = 9
ORDER = (
    tuple(range(9)) + (9, 10, 11, 12, 13),
    tuple(range(9)) + (10, 9, 11, 12, 13),
    tuple(range(9)) + (11, 9, 10, 12, 13),
)
NM = 9
T1, T2, EN, SC = 10, 11, 12, 13
CY, CU, CZ, CG, CC, CPHI, CRHO, CF = 0, 9, 12, 13, 14, 15, 24, 25
NCELL = 39
FINV, FWEIGHT, FSQUARE = 24, 25, 26
NFACE = 27
MESH = pl.DeviceIdType.MESH


def fill_table(nasa_ref, gas_ref, index_ref, tab_ref):
    for i in range(NS):
        k = index_ref[i]
        r = gas_ref[k]
        a = [nasa_ref[n, k] for n in range(6)]
        tab_ref[i, 0] = r
        tab_ref[i, 1] = r * (a[0] - 1.0)
        tab_ref[i, 2] = r * a[1]
        tab_ref[i, 3] = r * a[2]
        tab_ref[i, 4] = r * a[3]
        tab_ref[i, 5] = r * a[4]
        tab_ref[i, 6] = r * a[5]
        tab_ref[i, 7] = r * a[1] * 0.5
        tab_ref[i, 8] = r * a[2] * (1.0 / 3.0)
        tab_ref[i, 9] = r * a[3] * 0.25
        tab_ref[i, 10] = r * a[4] * 0.2


def cell_row(u, tab_ref):
    rho = u[0]
    for i in range(1, NS):
        rho = rho + u[i]
    inv = 1.0 / rho
    square = u[NM] * u[NM] + u[T1] * u[T1] + u[T2] * u[T2]
    energy = u[EN] - 0.5 * square * inv
    moment = []
    for n in range(7):
        total = u[0] * tab_ref[0, n]
        for i in range(1, NS):
            total = total + u[i] * tab_ref[i, n]
        moment.append(total)
    gas, k1, k2, k3, k4, k5, k6 = moment
    l2, l3, l4, l5 = k2 * 0.5, k3 * (1.0 / 3.0), k4 * 0.25, k5 * 0.2
    base = k6 - energy
    t = 1.0
    for _ in range(NEWTON):
        f = base + t * (k1 + t * (l2 + t * (l3 + t * (l4 + t * l5))))
        slope = k1 + t * (k2 + t * (k3 + t * (k4 + t * k5)))
        t = t - f / slope
    heat = k1 + t * (k2 + t * (k3 + t * (k4 + t * k5)))
    g = gas / heat
    p = gas * t
    c = jnp.sqrt((1.0 + g) * p * inv)
    half_q = 0.5 * square * inv * inv
    half_g, half_t = 0.5 * g, 0.5 * t
    phi = []
    for i in range(NS):
        e = tab_ref[i, 6] + t * (
            tab_ref[i, 1]
            + t * (tab_ref[i, 7] + t * (tab_ref[i, 8] + t * (tab_ref[i, 9] + t * tab_ref[i, 10])))
        )
        phi.append(tab_ref[i, 0] * half_t - half_g * (e - half_q))
    half_inv = 0.5 * inv
    cell = [u[i] * inv for i in range(NS)]
    cell += [u[k] * half_inv for k in (NM, T1, T2)]
    cell += [u[SC] * inv, half_g, 0.5 * c] + phi + [rho]
    v = u[NM] * inv
    flux = [u[k] * v for k in range(NVAR)]
    flux[NM] = flux[NM] + p
    flux[EN] = (u[EN] + p) * v
    cell += flux
    speed = [jnp.abs(u[k] * inv) + c for k in (NM, T1, T2)]
    return cell, speed


def correction(d0, d1, d2, d3):
    eps = 3.0 * EPSILON
    c0, c1, c2 = d1 - d0, d2 - d1, d3 - d2
    m1, m2 = 0.375 * d1, 0.375 * d2
    k1, k2 = (13.0 / 3.0) * (m1 * m1) + eps, (13.0 / 3.0) * (m2 * m2) + eps
    y0, y1, y2 = c0 + m1, c1 - m2, c2 - m2
    r0, r1, r2 = 1.0 / (y0 * y0 + k1), 1.0 / (y1 * y1 + k2), 1.0 / (y2 * y2 + k2)
    w0, w1, w2 = r0 * r0, r1 * r1, 3.0 * (r2 * r2)
    x0 = w0 * (c1 - c0)
    number = (x0 + x0) + w2 * (c2 - c1)
    total = (w0 + w2) + 6.0 * w1
    return number / total


def dot(a, b):
    return functools.reduce(lambda s, n: s + a[n] * b[n], range(1, len(a)), a[0] * b[0])


def face_means(first, f, cq):
    low, high = first + f + 2, first + f + 3
    mean = [cq[low, n] + cq[high, n] for n in range(CRHO)]
    y, phi = mean[CY : CY + NS], mean[CPHI : CPHI + NS]
    vn, v1, v2 = mean[CU : CU + 3]
    g, c = mean[CG], mean[CC]
    return mean + [1.0 / g, c * c - 0.5 * dot(y, phi), vn * vn + v1 * v1 + v2 * v2]


def splitter(mean):
    y, phi = mean[CY : CY + NS], mean[CPHI : CPHI + NS]
    vn, v1, v2 = mean[CU : CU + 3]
    z, g, c = mean[CZ], mean[CG], mean[CC]
    half_over_c = 0.5 / c
    half_over_cc = 2.0 * half_over_c * half_over_c

    def split(d, total):
        work = vn * d[NM] + v1 * d[T1] + v2 * d[T2]
        dp = dot(phi, d[:NS]) + g * (d[EN] - work)
        a = dp * half_over_cc
        b = (d[NM] - vn * total) * half_over_c
        parts = [d[k] - y[k] * a for k in range(NS)]
        return parts + [a - b, d[T1] - v1 * total, d[T2] - v2 * total, a + b, d[SC] - z * a]

    return split


def assemble(wave, mean):
    species = [wave(k) for k in range(NS)]
    slow, shear1, shear2, fast, scalar = [wave(k) for k in range(NS, NVAR)]
    y, phi = mean[CY : CY + NS], mean[CPHI : CPHI + NS]
    vn, v1, v2 = mean[CU : CU + 3]
    acoustic = slow + fast
    half_acoustic = 0.5 * acoustic
    pull = mean[CC] * (fast - slow)
    carried = functools.reduce(lambda s, n: s + n, species, acoustic)
    energy = (
        (mean[FWEIGHT] * acoustic - dot(species, phi)) * mean[FINV]
        + mean[FSQUARE] * carried
        + vn * pull
        + v1 * shear1
        + v2 * shear2
    )
    rows = [species[k] + y[k] * half_acoustic for k in range(NS)]
    rows += [vn * carried + pull, v1 * carried + shear1, v2 * carried + shear2, energy]
    return rows + [mean[CZ] * half_acoustic + scalar]


def prepare(first, f, i, uq, cq, lf, lu, bf, bu, mean_ref):
    mean = face_means(first, f, cq)
    for n in range(NFACE):
        mean_ref[i, n] = mean[n]
    split = splitter(mean)
    for n in range(5):
        here, there = first + f + n, first + f + n + 1
        du = [uq[there, k] - uq[here, k] for k in range(NVAR)]
        df = [cq[there, CF + k] - cq[here, CF + k] for k in range(NVAR)]
        parts = split(du, cq[there, CRHO] - cq[here, CRHO])
        for k in range(NVAR):
            lu[i, n, k] = parts[k]
        parts = split(df, du[NM])
        for k in range(NVAR):
            lf[i, n, k] = parts[k]
    for k in range(NVAR):
        f0, f1, f2, f3 = [cq[first + f + n, CF + k] for n in (1, 2, 3, 4)]
        bf[i, k] = 7.0 * (f1 + f2) - (f0 + f3)
    for k in range(NVAR):
        u0, u1, u2, u3 = [uq[first + f + n, k] for n in (1, 2, 3, 4)]
        bu[i, k] = (u3 - u0) - 3.0 * (u2 - u1)


def finish(alpha, i, lf, lu, bf, bu, mean_ref, fx):
    def wave(k):
        l = [lf[i, n, k] for n in range(5)]
        a = [alpha * lu[i, n, k] for n in range(5)]
        plus = correction(*[l[n] + a[n] for n in (0, 1, 2, 3)])
        minus = correction(*[l[n] - a[n] for n in (4, 3, 2, 1)])
        return minus - plus

    rows = assemble(wave, [mean_ref[i, n] for n in range(NFACE)])
    for k in range(NVAR):
        fx[i, k] = (bf[i, k] + alpha * bu[i, k]) + rows[k]


def direct(alpha, first, f, i, uq, cq, fx):
    mean = face_means(first, f, cq)
    split = splitter(mean)
    row = first + f
    plus, minus = [[] for _ in range(4)], [[] for _ in range(4)]
    for k in range(NVAR + 1):
        if k < NVAR:
            l = [cq[row + n, CF + k] for n in range(6)]
            a = [alpha * uq[row + n, k] for n in range(6)]
        else:
            l = [uq[row + n, NM] for n in range(6)]
            a = [alpha * cq[row + n, CRHO] for n in range(6)]
        p = [l[n] + a[n] for n in range(5)]
        m = [l[n] - a[n] for n in range(1, 6)]
        dp = [p[n + 1] - p[n] for n in range(4)]
        dm = [m[n + 1] - m[n] for n in range(4)]
        for n in range(4):
            plus[n].append(dp[n])
            minus[n].append(dm[n])
        if k < NVAR:
            x = dp[2] - dm[1]
            fx[i, k] = 6.0 * (p[2] + m[2]) + ((dp[1] - dm[2]) + (x + x))
    plus = [split(d[:NVAR], d[NVAR]) for d in plus]
    minus = [split(d[:NVAR], d[NVAR]) for d in minus]

    def wave(k):
        return correction(*[minus[n][k] for n in (3, 2, 1, 0)]) - correction(*[plus[n][k] for n in (0, 1, 2, 3)])

    rows = assemble(wave, mean)
    for k in range(NVAR):
        fx[i, k] = fx[i, k] + rows[k]


def kernel(
    u_hbm, nasa_ref, gas_ref, index_ref, kind_ref, out_ref,
    u_ref, u_sem, tab, uq, cq, lf, lu, bf, bu, mean_ref, fx, tmp, alphas,
    mine, slots, halo_send, halo_recv, speed_send, speed_recv,
):
    gx, gy = lax.axis_index("gx"), lax.axis_index("gy")
    nx, ny = lax.axis_size("gx"), lax.axis_size("gy")
    z, y_low, plane, core = gx // 2, gx % 2, gy // 2, gy % 2
    nz, n_plane = nx // 2, ny // 2
    x, y_high = plane // 2, plane % 2
    flat_steps = sorted(
        ((dx, high, low) for dx in range(n_plane // 2) for high in (0, 1) for low in (0, 1)),
        key=lambda d: -min(d[0], n_plane // 2 - d[0]) - (0, 1, 2, 1)[2 * d[1] + d[2]],
    )[:-1]
    tall_steps = sorted(range(1, nz), key=lambda d: -min(d, nz - d))

    def flat(step, sign, to_core):
        dx, high, low = step
        to_low, to_high = (y_low + low) % 2, (y_high + high) % 2
        to_x = (x + sign * dx + n_plane // 2) % (n_plane // 2)
        return (2 * z + to_low, 4 * to_x + 2 * to_high + to_core), 4 * to_x + 2 * to_high + to_low

    def tall(step, sign, to_core):
        to_z = (z + sign * step + nz) % nz
        return (2 * to_z + y_low, 2 * plane + to_core), to_z

    chip = 4 * x + 2 * y_high + y_low
    beside = [
        ((gx + nx - 1 + 2 * y_low) % nx, gy),
        (gx + 1 - 2 * y_low, gy),
        (gx, (gy + 1) % ny),
        (gx, (gy + ny - 1) % ny),
    ]
    load = pltpu.make_async_copy(u_hbm, u_ref, u_sem)
    load.start()
    barrier = pltpu.get_barrier_semaphore()

    def greet(peer):
        pl.semaphore_signal(barrier, inc=1, device_id=peer, device_id_type=MESH)

    @pl.when(core == 1)
    def _():
        for step in flat_steps:
            greet(flat(step, -1, 0)[0])
            greet(flat(step, -1, 1)[0])
        greet((gx, gy - 1))

    for step in tall_steps:
        greet(tall(step, -1, 1)[0])
    for peer in beside:
        greet(peer)

    @pl.when(core == 0)
    def _():
        greet((gx, gy + 1))

    fill_table(nasa_ref, gas_ref, index_ref, tab)
    lane = lax.broadcasted_iota(jnp.int32, (8, 128), 1)
    sub = lax.broadcasted_iota(jnp.int32, (8, 128), 0)
    left = lane < 64
    yb, zb = ROWS, 2 * ROWS

    load.wait()
    for k in range(NVAR):
        for r in range(8):
            uq[3 + r, k] = u_ref[ORDER[0][k], 8 * r : 8 * r + 8, :]

    def cells(r):
        cell, speed = cell_row([uq[r, k] for k in range(NVAR)], tab)
        for n in range(NCELL):
            cq[r, n] = cell[n]
        return speed

    zero = jnp.zeros((8, 128), jnp.float32)
    best = lax.fori_loop(
        3, 11, lambda r, best: tuple(jnp.maximum(a, b) for a, b in zip(best, cells(r))), (zero, zero, zero)
    )
    row = jnp.zeros((1, 128), jnp.float32)
    for d in range(3):
        row = jnp.where(lane[:1] == d, jnp.max(best[d], keepdims=True), row)
    mine[0] = row

    for pair in range(NVAR // 2):
        a, b = 2 * pair, 2 * pair + 1
        turned = jnp.transpose(jnp.concatenate([u_ref[a], u_ref[b]], axis=0))
        for t in range(8):
            lo, hi = turned[8 * t : 8 * t + 8], turned[64 + 8 * t : 72 + 8 * t]
            tmp[a, 8 * t : 8 * t + 8, :] = jnp.where(left, lo, pltpu.roll(hi, 64, 1))
            tmp[b, 8 * t : 8 * t + 8, :] = jnp.where(left, pltpu.roll(lo, 64, 1), hi)
    low_wall, high_wall = kind_ref[0, 0, 0] == 1, kind_ref[0, 0, 1] == 1
    for k in range(NVAR):
        cz = ORDER[2][k]
        rows = [tmp[cz, pl.ds(l, 8, stride=8), :] for l in range(8)]
        for l in range(8):
            uq[zb + 3 + l, k] = rows[l]
        sign = -1.0 if k == NM else 1.0
        for n in range(3):
            inside = pltpu.roll(rows[7 - n], 1, 0)
            ghost = jnp.where(low_wall, sign * rows[n], rows[0])
            edge = jnp.where(left, ghost, pltpu.roll(inside, 64, 1))
            uq[zb + 2 - n, k] = jnp.where(sub == 0, edge, inside)
            inside = pltpu.roll(rows[n], 7, 0)
            ghost = jnp.where(high_wall, sign * rows[7 - n], rows[7])
            edge = jnp.where(left, pltpu.roll(inside, 64, 1), ghost)
            uq[zb + 11 + n, k] = jnp.where(sub == 7, edge, inside)

    for k in range(NVAR):
        for r in range(8):
            uq[yb + 3 + r, k] = u_ref[ORDER[1][k], pl.ds(r, 8, stride=8), :]

    to_core_1 = len(flat_steps) + 2 * len(tall_steps) + 1 + len(beside)
    to_core_0 = len(flat_steps) + 1 + len(beside)

    @pl.when(core == 1)
    def _():
        pl.semaphore_wait(barrier, to_core_1)

    @pl.when(core == 0)
    def _():
        pl.semaphore_wait(barrier, to_core_0)


    def speed_copy(stage, n, slot, peer):
        return pltpu.make_async_remote_copy(
            src_ref=mine.at[stage],
            dst_ref=slots.at[stage, slot],
            send_sem=speed_send.at[stage, n],
            recv_sem=speed_recv.at[stage, slot],
            device_id=peer,
            device_id_type=MESH,
        )

    partner = (gx, gy + 1 - 2 * core)
    last = len(flat_steps)
    first_copies = [
        speed_copy(0, n, 2 * chip + core, flat(step, 1, 1)[0]) for n, step in enumerate(flat_steps)
    ]
    second_copies = [
        speed_copy(1, 2 * n + to_core, z, tall(step, 1, to_core)[0])
        for n, step in enumerate(tall_steps)
        for to_core in (0, 1)
    ] + [speed_copy(1, last, z, partner)]
    inward = speed_copy(0, last, 2 * chip + core, partner)

    for copy in first_copies:
        copy.start()

    @pl.when(core == 0)
    def _():
        inward.start()

    pieces = (
        (3 + 5 * y_low, 11 - 11 * y_low),
        (8 - 5 * y_low, 11 * y_low),
        (yb + 8, yb),
        (yb + 3, yb + 11),
    )
    halos = [
        pltpu.make_async_remote_copy(
            src_ref=uq.at[pl.ds(source, 3)],
            dst_ref=uq.at[pl.ds(target, 3)],
            send_sem=halo_send.at[n],
            recv_sem=halo_recv.at[n],
            device_id=beside[n],
            device_id_type=MESH,
        )
        for n, (source, target) in enumerate(pieces)
    ]
    halos[0].start()

    def before(first, f, i):
        prepare(first, f, i, uq, cq, lf, lu, bf, bu, mean_ref)

    @pl.loop(zb, zb + ROWS)
    def _(r):
        cells(r)

    @pl.loop(yb + 3, yb + 11)
    def _(r):
        cells(r)

    halos[1].start()
    @pl.loop(0, FACES)
    def _(f):
        before(zb, f, 2 * FACES + f)

    @pl.when(core == 1)
    def _():
        places = [2 * flat(step, -1, 1)[1] + side for step in flat_steps for side in (0, 1)] + [2 * chip]
        for slot in places:
            speed_copy(0, 0, slot, partner).wait_recv()
        total = mine[0]
        for slot in places:
            total = jnp.maximum(total, slots[0, slot])
        mine[1] = total
        for copy in second_copies:
            copy.start()
        slots[1, z] = total

    halos[2].start()
    halos[3].start()

    @pl.loop(0, 6)
    def _(n):
        d = n // 3
        f = 3 + n - 3 * d
        before(ROWS * d, f, FACES * d + f)

    for step in tall_steps:
        speed_copy(1, 0, tall(step, -1, 1)[1], partner).wait_recv()

    @pl.when(core == 0)
    def _():
        speed_copy(1, 0, z, partner).wait_recv()

    speeds = slots[1, 0]
    for n in range(1, nz):
        speeds = jnp.maximum(speeds, slots[1, n])
    total = None
    for d in range(3):
        alpha = jnp.max(jnp.where(lane[:1] == d, speeds, 0.0), keepdims=True)
        alphas[d] = jnp.broadcast_to(alpha, (8, 128))
        total = alphas[d] if total is None else total + alphas[d]
    scale = (COURANT / 12.0) / total

    def after(d, i):
        finish(alphas[d], i, lf, lu, bf, bu, mean_ref, fx)

    @pl.loop(0, FACES + 6)
    def _(n):
        half = n // FACES
        m = n - FACES * half
        d = 2 * (1 - half) + half * (m // 3)
        after(d, FACES * d + (1 - half) * m + half * (3 + m - 3 * (m // 3)))

    halos[0].wait_recv()
    halos[1].wait_recv()

    @pl.loop(0, 3)
    def _(n):
        cells(n)
        cells(n + 11)

    @pl.loop(0, 6)
    def _(n):
        f = n + 3 * (n // 3)
        direct(alphas[0], 0, f, f, uq, cq, fx)

    halos[2].wait_recv()
    halos[3].wait_recv()

    @pl.loop(0, 3)
    def _(n):
        cells(yb + n)
        cells(yb + n + 11)

    @pl.loop(0, 6)
    def _(n):
        f = n + 3 * (n // 3)
        direct(alphas[1], yb, f, FACES + f, uq, cq, fx)


    for k in range(NVAR):
        for r in range(8):
            tmp[ORDER[1][k], 8 * r : 8 * r + 8, :] = fx[FACES + r, k] - fx[FACES + r + 1, k]
    for k in range(NVAR):
        for r in range(8):
            rate = (fx[r, k] - fx[r + 1, k]) + tmp[k, pl.ds(r, 8, stride=8), :]
            out_ref[k, 8 * r : 8 * r + 8, :] = rate
    for k in range(NVAR):
        for r in range(8):
            tmp[ORDER[2][k], 8 * r : 8 * r + 8, :] = fx[2 * FACES + r, k] - fx[2 * FACES + r + 1, k]
    for pair in range(NVAR // 2):
        a, b = 2 * pair, 2 * pair + 1
        low, high = [], []
        for t in range(8):
            ra = tmp[a, pl.ds(t, 8, stride=8), :]
            rb = tmp[b, pl.ds(t, 8, stride=8), :]
            low.append(jnp.where(left, ra, pltpu.roll(rb, 64, 1)))
            high.append(jnp.where(left, pltpu.roll(ra, 64, 1), rb))
        back = jnp.transpose(jnp.concatenate(low + high, axis=0))
        for r in range(8):
            here = slice(8 * r, 8 * r + 8)
            out_ref[a, here] = scale * (out_ref[a, here] + back[8 * r : 8 * r + 8])
            out_ref[b, here] = scale * (out_ref[b, here] + back[64 + 8 * r : 72 + 8 * r])

    for copy in halos:
        copy.wait_send()
    for copy in first_copies:
        copy.wait_send()

    @pl.when(core == 0)
    def _():
        inward.wait_send()

    @pl.when(core == 1)
    def _():
        for copy in second_copies:
            copy.wait_send()


def solution(mesh):
    def shards(u, nasa, gas, index, kind):
        vmem = pl.BlockSpec(memory_space=pltpu.VMEM)
        smem = pl.BlockSpec(memory_space=pltpu.SMEM)
        f32 = jnp.float32

        def rows(*lead):
            return pltpu.VMEM(lead + (8, 128), f32)

        out = pl.pallas_call(
            kernel,
            out_shape=jax.ShapeDtypeStruct((NVAR, 64, 128), f32),
            in_specs=[pl.BlockSpec(memory_space=pl.ANY)] + [smem] * 4,
            out_specs=vmem,
            scratch_shapes=[
                pltpu.VMEM((NVAR, 64, 128), f32),
                pltpu.SemaphoreType.DMA,
                pltpu.SMEM((NS, 11), f32),
                rows(3 * ROWS, NVAR),
                rows(3 * ROWS, NCELL),
                rows(3 * FACES, 5, NVAR),
                rows(3 * FACES, 5, NVAR),
                rows(3 * FACES, NVAR),
                rows(3 * FACES, NVAR),
                rows(3 * FACES, NFACE),
                rows(3 * FACES, NVAR),
                pltpu.VMEM((NVAR, 64, 128), f32),
                rows(3),
                pltpu.VMEM((2, 1, 128), f32),
                pltpu.VMEM((2, 32, 1, 128), f32),
                pltpu.SemaphoreType.DMA((4,)),
                pltpu.SemaphoreType.DMA((4,)),
                pltpu.SemaphoreType.DMA((2, 16)),
                pltpu.SemaphoreType.DMA((2, 32)),
            ],
            compiler_params=pltpu.CompilerParams(
                collective_id=0, has_side_effects=True, vmem_limit_bytes=36 * 1024 * 1024
            ),
        )(*[pltpu.with_memory_space_constraint(a, pltpu.HBM) for a in (u.reshape(NVAR, 64, 128), nasa.T, gas, index, kind)])
        return out.reshape(u.shape)

    whole = P(None, "gx", "gy", None)
    return jax.shard_map(
        shards, mesh=mesh, in_specs=(whole, P(), P(), P(), P("gx", "gy", None)), out_specs=whole, check_vma=False
    )
```

```python
import functools

import jax
import jax.numpy as jnp
from jax import lax
from jax.experimental import pallas as pl
from jax.experimental.pallas import tpu as pltpu
from jax.sharding import PartitionSpec as P

NS = 9
NVAR = 14
NEWTON = 2
EPSILON = 1e-06
COURANT = 0.8

ROWS = 14
FACES = 9
ORDER = (
    tuple(range(9)) + (9, 10, 11, 12, 13),
    tuple(range(9)) + (10, 9, 11, 12, 13),
    tuple(range(9)) + (11, 9, 10, 12, 13),
)
NM = 9
T1, T2, EN, SC = 10, 11, 12, 13
CY, CU, CZ, CG, CC, CPHI, CRHO, CF = 0, 9, 12, 13, 14, 15, 24, 25
NCELL = 39
FINV, FWEIGHT, FSQUARE = 24, 25, 26
NFACE = 27
MESH = pl.DeviceIdType.MESH


def fill_table(nasa_ref, gas_ref, index_ref, tab_ref):
    for i in range(NS):
        k = index_ref[i]
        r = gas_ref[k]
        a = [nasa_ref[n, k] for n in range(6)]
        tab_ref[i, 0] = r
        tab_ref[i, 1] = r * (a[0] - 1.0)
        tab_ref[i, 2] = r * a[1]
        tab_ref[i, 3] = r * a[2]
        tab_ref[i, 4] = r * a[3]
        tab_ref[i, 5] = r * a[4]
        tab_ref[i, 6] = r * a[5]
        tab_ref[i, 7] = r * a[1] * 0.5
        tab_ref[i, 8] = r * a[2] * (1.0 / 3.0)
        tab_ref[i, 9] = r * a[3] * 0.25
        tab_ref[i, 10] = r * a[4] * 0.2


def state_row(u, tab_ref):
    rho = u[0]
    for i in range(1, NS):
        rho = rho + u[i]
    inv = 1.0 / rho
    square = u[NM] * u[NM] + u[T1] * u[T1] + u[T2] * u[T2]
    energy = u[EN] - 0.5 * square * inv
    moment = []
    for n in range(7):
        total = u[0] * tab_ref[0, n]
        for i in range(1, NS):
            total = total + u[i] * tab_ref[i, n]
        moment.append(total)
    gas, k1, k2, k3, k4, k5, k6 = moment
    l2, l3, l4, l5 = k2 * 0.5, k3 * (1.0 / 3.0), k4 * 0.25, k5 * 0.2
    base = k6 - energy
    t = 1.0
    for _ in range(NEWTON):
        f = base + t * (k1 + t * (l2 + t * (l3 + t * (l4 + t * l5))))
        slope = k1 + t * (k2 + t * (k3 + t * (k4 + t * k5)))
        t = t - f / slope
    heat = k1 + t * (k2 + t * (k3 + t * (k4 + t * k5)))
    g = gas / heat
    p = gas * t
    c = jnp.sqrt((1.0 + g) * p * inv)
    return rho, inv, square, t, g, p, c


def speed_row(u, tab_ref):
    _, inv, _, _, _, _, c = state_row(u, tab_ref)
    return [jnp.abs(u[k] * inv) + c for k in (NM, T1, T2)]


def cell_row(u, tab_ref):
    rho, inv, square, t, g, p, c = state_row(u, tab_ref)
    half_q = 0.5 * square * inv * inv
    half_g, half_t = 0.5 * g, 0.5 * t
    phi = []
    for i in range(NS):
        e = tab_ref[i, 6] + t * (
            tab_ref[i, 1]
            + t * (tab_ref[i, 7] + t * (tab_ref[i, 8] + t * (tab_ref[i, 9] + t * tab_ref[i, 10])))
        )
        phi.append(tab_ref[i, 0] * half_t - half_g * (e - half_q))
    half_inv = 0.5 * inv
    cell = [u[i] * inv for i in range(NS)]
    cell += [u[k] * half_inv for k in (NM, T1, T2)]
    cell += [u[SC] * inv, half_g, 0.5 * c] + phi + [rho]
    v = u[NM] * inv
    flux = [u[k] * v for k in range(NVAR)]
    flux[NM] = flux[NM] + p
    flux[EN] = (u[EN] + p) * v
    cell += flux
    return cell


def correction(d0, d1, d2, d3):
    eps = 3.0 * EPSILON
    c0, c1, c2 = d1 - d0, d2 - d1, d3 - d2
    m1, m2 = 0.375 * d1, 0.375 * d2
    k1, k2 = (13.0 / 3.0) * (m1 * m1) + eps, (13.0 / 3.0) * (m2 * m2) + eps
    y0, y1, y2 = c0 + m1, c1 - m2, c2 - m2
    r0, r1, r2 = 1.0 / (y0 * y0 + k1), 1.0 / (y1 * y1 + k2), 1.0 / (y2 * y2 + k2)
    w0, w1, w2 = r0 * r0, r1 * r1, 3.0 * (r2 * r2)
    x0 = w0 * (c1 - c0)
    number = (x0 + x0) + w2 * (c2 - c1)
    total = (w0 + w2) + 6.0 * w1
    return number / total


def dot(a, b):
    return functools.reduce(lambda s, n: s + a[n] * b[n], range(1, len(a)), a[0] * b[0])


def face_means(first, f, cq):
    low, high = first + f + 2, first + f + 3
    mean = [cq[low, n] + cq[high, n] for n in range(CRHO)]
    y, phi = mean[CY : CY + NS], mean[CPHI : CPHI + NS]
    vn, v1, v2 = mean[CU : CU + 3]
    g, c = mean[CG], mean[CC]
    return mean + [1.0 / g, c * c - 0.5 * dot(y, phi), vn * vn + v1 * v1 + v2 * v2]


def splitter(mean):
    y, phi = mean[CY : CY + NS], mean[CPHI : CPHI + NS]
    vn, v1, v2 = mean[CU : CU + 3]
    z, g, c = mean[CZ], mean[CG], mean[CC]
    half_over_c = 0.5 / c
    half_over_cc = 2.0 * half_over_c * half_over_c

    def split(d, total):
        work = vn * d[NM] + v1 * d[T1] + v2 * d[T2]
        dp = dot(phi, d[:NS]) + g * (d[EN] - work)
        a = dp * half_over_cc
        b = (d[NM] - vn * total) * half_over_c
        parts = [d[k] - y[k] * a for k in range(NS)]
        return parts + [a - b, d[T1] - v1 * total, d[T2] - v2 * total, a + b, d[SC] - z * a]

    return split


def assemble(wave, mean):
    species = [wave(k) for k in range(NS)]
    slow, shear1, shear2, fast, scalar = [wave(k) for k in range(NS, NVAR)]
    y, phi = mean[CY : CY + NS], mean[CPHI : CPHI + NS]
    vn, v1, v2 = mean[CU : CU + 3]
    acoustic = slow + fast
    half_acoustic = 0.5 * acoustic
    pull = mean[CC] * (fast - slow)
    carried = functools.reduce(lambda s, n: s + n, species, acoustic)
    energy = (
        (mean[FWEIGHT] * acoustic - dot(species, phi)) * mean[FINV]
        + mean[FSQUARE] * carried
        + vn * pull
        + v1 * shear1
        + v2 * shear2
    )
    rows = [species[k] + y[k] * half_acoustic for k in range(NS)]
    rows += [vn * carried + pull, v1 * carried + shear1, v2 * carried + shear2, energy]
    return rows + [mean[CZ] * half_acoustic + scalar]


def prepare(first, f, i, uq, cq, lf, lu, bf, bu, mean_ref, places=(0, 1, 2, 3, 4), linear=True, fresh=True):
    if fresh:
        mean = face_means(first, f, cq)
        for n in range(NFACE):
            mean_ref[i, n] = mean[n]
    else:
        mean = [mean_ref[i, n] for n in range(NFACE)]
    split = splitter(mean)
    for n in places:
        here, there = first + f + n, first + f + n + 1
        du = [uq[there, k] - uq[here, k] for k in range(NVAR)]
        df = [cq[there, CF + k] - cq[here, CF + k] for k in range(NVAR)]
        parts = split(du, cq[there, CRHO] - cq[here, CRHO])
        for k in range(NVAR):
            lu[i, n, k] = parts[k]
        parts = split(df, du[NM])
        for k in range(NVAR):
            lf[i, n, k] = parts[k]
    if not linear:
        return
    for k in range(NVAR):
        f0, f1, f2, f3 = [cq[first + f + n, CF + k] for n in (1, 2, 3, 4)]
        bf[i, k] = 7.0 * (f1 + f2) - (f0 + f3)
    for k in range(NVAR):
        u0, u1, u2, u3 = [uq[first + f + n, k] for n in (1, 2, 3, 4)]
        bu[i, k] = (u3 - u0) - 3.0 * (u2 - u1)


def finish(alpha, i, lf, lu, bf, bu, mean_ref, fx):
    def wave(k):
        l = [lf[i, n, k] for n in range(5)]
        a = [alpha * lu[i, n, k] for n in range(5)]
        plus = correction(*[l[n] + a[n] for n in (0, 1, 2, 3)])
        minus = correction(*[l[n] - a[n] for n in (4, 3, 2, 1)])
        return minus - plus

    rows = assemble(wave, [mean_ref[i, n] for n in range(NFACE)])
    for k in range(NVAR):
        fx[i, k] = (bf[i, k] + alpha * bu[i, k]) + rows[k]


def direct(alpha, first, f, i, uq, cq, fx):
    mean = face_means(first, f, cq)
    split = splitter(mean)
    row = first + f
    plus, minus = [[] for _ in range(4)], [[] for _ in range(4)]
    for k in range(NVAR + 1):
        if k < NVAR:
            l = [cq[row + n, CF + k] for n in range(6)]
            a = [alpha * uq[row + n, k] for n in range(6)]
        else:
            l = [uq[row + n, NM] for n in range(6)]
            a = [alpha * cq[row + n, CRHO] for n in range(6)]
        p = [l[n] + a[n] for n in range(5)]
        m = [l[n] - a[n] for n in range(1, 6)]
        dp = [p[n + 1] - p[n] for n in range(4)]
        dm = [m[n + 1] - m[n] for n in range(4)]
        for n in range(4):
            plus[n].append(dp[n])
            minus[n].append(dm[n])
        if k < NVAR:
            x = dp[2] - dm[1]
            fx[i, k] = 6.0 * (p[2] + m[2]) + ((dp[1] - dm[2]) + (x + x))
    plus = [split(d[:NVAR], d[NVAR]) for d in plus]
    minus = [split(d[:NVAR], d[NVAR]) for d in minus]

    def wave(k):
        return correction(*[minus[n][k] for n in (3, 2, 1, 0)]) - correction(*[plus[n][k] for n in (0, 1, 2, 3)])

    rows = assemble(wave, mean)
    for k in range(NVAR):
        fx[i, k] = fx[i, k] + rows[k]


def kernel(
    u_hbm, nasa_ref, gas_ref, index_ref, kind_ref, out_ref,
    u_ref, u_sem, tab, uq, cq, lf, lu, bf, bu, mean_ref, fx, tmp, alphas,
    mine, slots, halo_send, halo_recv, speed_send, speed_recv,
):
    gx, gy = lax.axis_index("gx"), lax.axis_index("gy")
    nx, ny = lax.axis_size("gx"), lax.axis_size("gy")
    z, y_low, plane, core = gx // 2, gx % 2, gy // 2, gy % 2
    nz, n_plane = nx // 2, ny // 2
    x, y_high = plane // 2, plane % 2
    flat_steps = sorted(
        ((dx, high, low) for dx in range(n_plane // 2) for high in (0, 1) for low in (0, 1)),
        key=lambda d: -min(d[0], n_plane // 2 - d[0]) - (0, 1, 2, 1)[2 * d[1] + d[2]],
    )[:-1]
    tall_steps = sorted(range(1, nz), key=lambda d: -min(d, nz - d))

    def flat(step, sign, to_core):
        dx, high, low = step
        to_low, to_high = (y_low + low) % 2, (y_high + high) % 2
        to_x = (x + sign * dx + n_plane // 2) % (n_plane // 2)
        return (2 * z + to_low, 4 * to_x + 2 * to_high + to_core), 4 * to_x + 2 * to_high + to_low

    def tall(step, sign, to_core):
        to_z = (z + sign * step + nz) % nz
        return (2 * to_z + y_low, 2 * plane + to_core), to_z

    chip = 4 * x + 2 * y_high + y_low
    beside = [
        ((gx + nx - 1 + 2 * y_low) % nx, gy),
        (gx + 1 - 2 * y_low, gy),
        (gx, (gy + 1) % ny),
        (gx, (gy + ny - 1) % ny),
    ]
    load = pltpu.make_async_copy(u_hbm, u_ref, u_sem)
    load.start()
    barrier = pltpu.get_barrier_semaphore()

    def greet(peer):
        pl.semaphore_signal(barrier, inc=1, device_id=peer, device_id_type=MESH)

    @pl.when(core == 1)
    def _():
        for step in flat_steps:
            greet(flat(step, -1, 0)[0])
            greet(flat(step, -1, 1)[0])
        greet((gx, gy - 1))

    for step in tall_steps:
        greet(tall(step, -1, 1)[0])
    for peer in beside:
        greet(peer)

    @pl.when(core == 0)
    def _():
        greet((gx, gy + 1))

    fill_table(nasa_ref, gas_ref, index_ref, tab)
    lane = lax.broadcasted_iota(jnp.int32, (8, 128), 1)
    sub = lax.broadcasted_iota(jnp.int32, (8, 128), 0)
    left = lane < 64
    yb, zb = ROWS, 2 * ROWS

    load.wait()
    for k in range(NVAR):
        for r in range(8):
            uq[3 + r, k] = u_ref[ORDER[0][k], 8 * r : 8 * r + 8, :]

    def cells(r):
        cell = cell_row([uq[r, k] for k in range(NVAR)], tab)
        for n in range(NCELL):
            cq[r, n] = cell[n]

    def speeds_with(r, best):
        speed = speed_row([uq[r, k] for k in range(NVAR)], tab)
        return tuple(jnp.maximum(a, b) for a, b in zip(best, speed))

    zero = jnp.zeros((8, 128), jnp.float32)
    best = lax.fori_loop(
        0, 4, lambda n, best: speeds_with(2 * n + 4, speeds_with(2 * n + 3, best)), (zero, zero, zero)
    )
    row = jnp.zeros((1, 128), jnp.float32)
    for d in range(3):
        row = jnp.where(lane[:1] == d, jnp.max(best[d], keepdims=True), row)
    mine[0] = row

    to_core_1 = len(flat_steps) + 2 * len(tall_steps) + 1 + len(beside)
    to_core_0 = len(flat_steps) + 1 + len(beside)

    @pl.when(core == 1)
    def _():
        pl.semaphore_wait(barrier, to_core_1)

    @pl.when(core == 0)
    def _():
        pl.semaphore_wait(barrier, to_core_0)


    def speed_copy(stage, n, slot, peer):
        return pltpu.make_async_remote_copy(
            src_ref=mine.at[stage],
            dst_ref=slots.at[stage, slot],
            send_sem=speed_send.at[stage, n],
            recv_sem=speed_recv.at[stage, slot],
            device_id=peer,
            device_id_type=MESH,
        )

    partner = (gx, gy + 1 - 2 * core)
    last = len(flat_steps)
    first_copies = [
        speed_copy(0, n, 2 * chip + core, flat(step, 1, 1)[0]) for n, step in enumerate(flat_steps)
    ]
    second_copies = [
        speed_copy(1, 2 * n + to_core, z, tall(step, 1, to_core)[0])
        for n, step in enumerate(tall_steps)
        for to_core in (0, 1)
    ] + [speed_copy(1, last, z, partner)]
    inward = speed_copy(0, last, 2 * chip + core, partner)

    for copy in first_copies:
        copy.start()

    @pl.when(core == 0)
    def _():
        inward.start()

    pieces = (
        (3 + 5 * y_low, 11 - 11 * y_low),
        (8 - 5 * y_low, 11 * y_low),
        (yb + 8, yb),
        (yb + 3, yb + 11),
    )
    halos = [
        pltpu.make_async_remote_copy(
            src_ref=uq.at[pl.ds(source, 3)],
            dst_ref=uq.at[pl.ds(target, 3)],
            send_sem=halo_send.at[n],
            recv_sem=halo_recv.at[n],
            device_id=beside[n],
            device_id_type=MESH,
        )
        for n, (source, target) in enumerate(pieces)
    ]
    halos[0].start()

    for pair in range(NVAR // 2):
        a, b = 2 * pair, 2 * pair + 1
        turned = jnp.transpose(jnp.concatenate([u_ref[a], u_ref[b]], axis=0))
        for t in range(8):
            lo, hi = turned[8 * t : 8 * t + 8], turned[64 + 8 * t : 72 + 8 * t]
            tmp[a, 8 * t : 8 * t + 8, :] = jnp.where(left, lo, pltpu.roll(hi, 64, 1))
            tmp[b, 8 * t : 8 * t + 8, :] = jnp.where(left, pltpu.roll(lo, 64, 1), hi)
    low_wall, high_wall = kind_ref[0, 0, 0] == 1, kind_ref[0, 0, 1] == 1
    for k in range(NVAR):
        cz = ORDER[2][k]
        rows = [tmp[cz, pl.ds(l, 8, stride=8), :] for l in range(8)]
        for l in range(8):
            uq[zb + 3 + l, k] = rows[l]
        sign = -1.0 if k == NM else 1.0
        for n in range(3):
            inside = pltpu.roll(rows[7 - n], 1, 0)
            ghost = jnp.where(low_wall, sign * rows[n], rows[0])
            edge = jnp.where(left, ghost, pltpu.roll(inside, 64, 1))
            uq[zb + 2 - n, k] = jnp.where(sub == 0, edge, inside)
            inside = pltpu.roll(rows[n], 7, 0)
            ghost = jnp.where(high_wall, sign * rows[7 - n], rows[7])
            edge = jnp.where(left, pltpu.roll(inside, 64, 1), ghost)
            uq[zb + 11 + n, k] = jnp.where(sub == 7, edge, inside)

    for k in range(NVAR):
        for r in range(8):
            uq[yb + 3 + r, k] = u_ref[ORDER[1][k], pl.ds(r, 8, stride=8), :]

    def before(first, f, i, *how):
        prepare(first, f, i, uq, cq, lf, lu, bf, bu, mean_ref, *how)

    def rest(d):
        for f, places, linear in ((1, (0, 1), True), (2, (0,), False), (6, (4,), False), (7, (3, 4), True)):
            before(ROWS * d, f, FACES * d + f, places, linear, False)

        @pl.loop(0, 2)
        def _(n):
            direct(alphas[d], ROWS * d, 8 * n, FACES * d + 8 * n, uq, cq, fx)

        @pl.loop(0, 4)
        def _(n):
            after(d, FACES * d + 1 + n + 3 * (n // 2))

    @pl.loop(zb, zb + ROWS)
    def _(r):
        cells(r)

    @pl.loop(yb + 3, yb + 11)
    def _(r):
        cells(r)

    halos[1].start()
    @pl.loop(0, FACES)
    def _(f):
        before(zb, f, 2 * FACES + f)

    @pl.when(core == 1)
    def _():
        places = [2 * flat(step, -1, 1)[1] + side for step in flat_steps for side in (0, 1)] + [2 * chip]
        for slot in places:
            speed_copy(0, 0, slot, partner).wait_recv()
        total = mine[0]
        for slot in places:
            total = jnp.maximum(total, slots[0, slot])
        mine[1] = total
        for copy in second_copies:
            copy.start()
        slots[1, z] = total

    halos[2].start()
    halos[3].start()

    @pl.loop(0, 4)
    def _(n):
        cells(2 * n + 3)
        cells(2 * n + 4)

    @pl.loop(0, 6)
    def _(n):
        d = n // 3
        f = 3 + n - 3 * d
        before(ROWS * d, f, FACES * d + f)

    @pl.loop(0, 2)
    def _(d):
        for f, places, linear in (
            (1, (2, 3, 4), False),
            (2, (1, 2, 3, 4), True),
            (6, (0, 1, 2, 3), True),
            (7, (0, 1, 2), False),
        ):
            before(ROWS * d, f, FACES * d + f, places, linear)

    for step in tall_steps:
        speed_copy(1, 0, tall(step, -1, 1)[1], partner).wait_recv()

    @pl.when(core == 0)
    def _():
        speed_copy(1, 0, z, partner).wait_recv()

    speeds = slots[1, 0]
    for n in range(1, nz):
        speeds = jnp.maximum(speeds, slots[1, n])
    total = None
    for d in range(3):
        alpha = jnp.max(jnp.where(lane[:1] == d, speeds, 0.0), keepdims=True)
        alphas[d] = jnp.broadcast_to(alpha, (8, 128))
        total = alphas[d] if total is None else total + alphas[d]
    scale = (COURANT / 12.0) / total

    def after(d, i):
        finish(alphas[d], i, lf, lu, bf, bu, mean_ref, fx)

    @pl.loop(0, FACES + 6)
    def _(n):
        half = n // FACES
        m = n - FACES * half
        d = 2 * (1 - half) + half * (m // 3)
        after(d, FACES * d + (1 - half) * m + half * (3 + m - 3 * (m // 3)))

    halos[0].wait_recv()
    halos[1].wait_recv()

    @pl.loop(0, 3)
    def _(n):
        cells(n)
        cells(n + 11)

    rest(0)

    halos[2].wait_recv()
    halos[3].wait_recv()

    @pl.loop(0, 3)
    def _(n):
        cells(yb + n)
        cells(yb + n + 11)

    rest(1)


    for k in range(NVAR):
        for r in range(8):
            tmp[ORDER[1][k], 8 * r : 8 * r + 8, :] = fx[FACES + r, k] - fx[FACES + r + 1, k]
    for k in range(NVAR):
        for r in range(8):
            rate = (fx[r, k] - fx[r + 1, k]) + tmp[k, pl.ds(r, 8, stride=8), :]
            out_ref[k, 8 * r : 8 * r + 8, :] = rate
    for k in range(NVAR):
        for r in range(8):
            tmp[ORDER[2][k], 8 * r : 8 * r + 8, :] = fx[2 * FACES + r, k] - fx[2 * FACES + r + 1, k]
    for pair in range(NVAR // 2):
        a, b = 2 * pair, 2 * pair + 1
        low, high = [], []
        for t in range(8):
            ra = tmp[a, pl.ds(t, 8, stride=8), :]
            rb = tmp[b, pl.ds(t, 8, stride=8), :]
            low.append(jnp.where(left, ra, pltpu.roll(rb, 64, 1)))
            high.append(jnp.where(left, pltpu.roll(ra, 64, 1), rb))
        back = jnp.transpose(jnp.concatenate(low + high, axis=0))
        for r in range(8):
            here = slice(8 * r, 8 * r + 8)
            out_ref[a, here] = scale * (out_ref[a, here] + back[8 * r : 8 * r + 8])
            out_ref[b, here] = scale * (out_ref[b, here] + back[64 + 8 * r : 72 + 8 * r])

    for copy in halos:
        copy.wait_send()
    for copy in first_copies:
        copy.wait_send()

    @pl.when(core == 0)
    def _():
        inward.wait_send()

    @pl.when(core == 1)
    def _():
        for copy in second_copies:
            copy.wait_send()


def solution(mesh):
    def shards(u, nasa, gas, index, kind):
        vmem = pl.BlockSpec(memory_space=pltpu.VMEM)
        smem = pl.BlockSpec(memory_space=pltpu.SMEM)
        f32 = jnp.float32

        def rows(*lead):
            return pltpu.VMEM(lead + (8, 128), f32)

        out = pl.pallas_call(
            kernel,
            out_shape=jax.ShapeDtypeStruct((NVAR, 64, 128), f32),
            in_specs=[pl.BlockSpec(memory_space=pl.ANY)] + [smem] * 4,
            out_specs=vmem,
            scratch_shapes=[
                pltpu.VMEM((NVAR, 64, 128), f32),
                pltpu.SemaphoreType.DMA,
                pltpu.SMEM((NS, 11), f32),
                rows(3 * ROWS, NVAR),
                rows(3 * ROWS, NCELL),
                rows(3 * FACES, 5, NVAR),
                rows(3 * FACES, 5, NVAR),
                rows(3 * FACES, NVAR),
                rows(3 * FACES, NVAR),
                rows(3 * FACES, NFACE),
                rows(3 * FACES, NVAR),
                pltpu.VMEM((NVAR, 64, 128), f32),
                rows(3),
                pltpu.VMEM((2, 1, 128), f32),
                pltpu.VMEM((2, 32, 1, 128), f32),
                pltpu.SemaphoreType.DMA((4,)),
                pltpu.SemaphoreType.DMA((4,)),
                pltpu.SemaphoreType.DMA((2, 16)),
                pltpu.SemaphoreType.DMA((2, 32)),
            ],
            compiler_params=pltpu.CompilerParams(
                collective_id=0, has_side_effects=True, vmem_limit_bytes=36 * 1024 * 1024
            ),
        )(*[pltpu.with_memory_space_constraint(a, pltpu.HBM) for a in (u.reshape(NVAR, 64, 128), nasa.T, gas, index, kind)])
        return out.reshape(u.shape)

    whole = P(None, "gx", "gy", None)
    return jax.shard_map(
        shards, mesh=mesh, in_specs=(whole, P(), P(), P(), P("gx", "gy", None)), out_specs=whole, check_vma=False
    )
```

```python
import functools

import jax
import jax.numpy as jnp
from jax import lax
from jax.experimental import pallas as pl
from jax.experimental.pallas import tpu as pltpu
from jax.sharding import PartitionSpec as P

NS = 9
NVAR = 14
NEWTON = 2
EPSILON = 1e-06
COURANT = 0.8

ROWS = 14
FACES = 9
ORDER = (
    tuple(range(9)) + (9, 10, 11, 12, 13),
    tuple(range(9)) + (10, 9, 11, 12, 13),
    tuple(range(9)) + (11, 9, 10, 12, 13),
)
NM = 9
T1, T2, EN, SC = 10, 11, 12, 13
CY, CU, CZ, CG, CC, CPHI, CRHO, CF = 0, 9, 12, 13, 14, 15, 24, 25
NCELL = 39
FINV, FWEIGHT, FSQUARE = 24, 25, 26
NFACE = 27
MESH = pl.DeviceIdType.MESH


def fill_table(nasa_ref, gas_ref, index_ref, tab_ref):
    for i in range(NS):
        k = index_ref[i]
        r = gas_ref[k]
        a = [nasa_ref[n, k] for n in range(6)]
        tab_ref[i, 0] = r
        tab_ref[i, 1] = r * (a[0] - 1.0)
        tab_ref[i, 2] = r * a[1]
        tab_ref[i, 3] = r * a[2]
        tab_ref[i, 4] = r * a[3]
        tab_ref[i, 5] = r * a[4]
        tab_ref[i, 6] = r * a[5]
        tab_ref[i, 7] = r * a[1] * 0.5
        tab_ref[i, 8] = r * a[2] * (1.0 / 3.0)
        tab_ref[i, 9] = r * a[3] * 0.25
        tab_ref[i, 10] = r * a[4] * 0.2


def state_row(u, tab_ref):
    rho = u[0]
    for i in range(1, NS):
        rho = rho + u[i]
    inv = 1.0 / rho
    square = u[NM] * u[NM] + u[T1] * u[T1] + u[T2] * u[T2]
    energy = u[EN] - 0.5 * square * inv
    moment = []
    for n in range(7):
        total = u[0] * tab_ref[0, n]
        for i in range(1, NS):
            total = total + u[i] * tab_ref[i, n]
        moment.append(total)
    gas, k1, k2, k3, k4, k5, k6 = moment
    l2, l3, l4, l5 = k2 * 0.5, k3 * (1.0 / 3.0), k4 * 0.25, k5 * 0.2
    base = k6 - energy
    t = 1.0
    for _ in range(NEWTON):
        f = base + t * (k1 + t * (l2 + t * (l3 + t * (l4 + t * l5))))
        slope = k1 + t * (k2 + t * (k3 + t * (k4 + t * k5)))
        t = t - f / slope
    heat = k1 + t * (k2 + t * (k3 + t * (k4 + t * k5)))
    g = gas / heat
    p = gas * t
    c = jnp.sqrt((1.0 + g) * p * inv)
    return rho, inv, square, t, g, p, c


def speed_row(u, tab_ref):
    _, inv, _, _, _, _, c = state_row(u, tab_ref)
    return [jnp.abs(u[k] * inv) + c for k in (NM, T1, T2)]


def cell_row(u, tab_ref):
    rho, inv, square, t, g, p, c = state_row(u, tab_ref)
    half_q = 0.5 * square * inv * inv
    half_g, half_t = 0.5 * g, 0.5 * t
    phi = []
    for i in range(NS):
        e = tab_ref[i, 6] + t * (
            tab_ref[i, 1]
            + t * (tab_ref[i, 7] + t * (tab_ref[i, 8] + t * (tab_ref[i, 9] + t * tab_ref[i, 10])))
        )
        phi.append(tab_ref[i, 0] * half_t - half_g * (e - half_q))
    half_inv = 0.5 * inv
    cell = [u[i] * inv for i in range(NS)]
    cell += [u[k] * half_inv for k in (NM, T1, T2)]
    cell += [u[SC] * inv, half_g, 0.5 * c] + phi + [rho]
    v = u[NM] * inv
    flux = [u[k] * v for k in range(NVAR)]
    flux[NM] = flux[NM] + p
    flux[EN] = (u[EN] + p) * v
    cell += flux
    return cell


def correction(d0, d1, d2, d3):
    eps = 3.0 * EPSILON
    c0, c1, c2 = d1 - d0, d2 - d1, d3 - d2
    m1, m2 = 0.375 * d1, 0.375 * d2
    k1, k2 = (13.0 / 3.0) * (m1 * m1) + eps, (13.0 / 3.0) * (m2 * m2) + eps
    y0, y1, y2 = c0 + m1, c1 - m2, c2 - m2
    r0, r1, r2 = 1.0 / (y0 * y0 + k1), 1.0 / (y1 * y1 + k2), 1.0 / (y2 * y2 + k2)
    w0, w1, w2 = r0 * r0, r1 * r1, 3.0 * (r2 * r2)
    x0 = w0 * (c1 - c0)
    number = (x0 + x0) + w2 * (c2 - c1)
    total = (w0 + w2) + 6.0 * w1
    return number / total


def dot(a, b):
    return functools.reduce(lambda s, n: s + a[n] * b[n], range(1, len(a)), a[0] * b[0])


def face_means(first, f, cq):
    low, high = first + f + 2, first + f + 3
    mean = [cq[low, n] + cq[high, n] for n in range(CRHO)]
    y, phi = mean[CY : CY + NS], mean[CPHI : CPHI + NS]
    vn, v1, v2 = mean[CU : CU + 3]
    g, c = mean[CG], mean[CC]
    return mean + [1.0 / g, c * c - 0.5 * dot(y, phi), vn * vn + v1 * v1 + v2 * v2]


def splitter(mean):
    y, phi = mean[CY : CY + NS], mean[CPHI : CPHI + NS]
    vn, v1, v2 = mean[CU : CU + 3]
    z, g, c = mean[CZ], mean[CG], mean[CC]
    half_over_c = 0.5 / c
    half_over_cc = 2.0 * half_over_c * half_over_c

    def split(d, total):
        work = vn * d[NM] + v1 * d[T1] + v2 * d[T2]
        dp = dot(phi, d[:NS]) + g * (d[EN] - work)
        a = dp * half_over_cc
        b = (d[NM] - vn * total) * half_over_c
        parts = [d[k] - y[k] * a for k in range(NS)]
        return parts + [a - b, d[T1] - v1 * total, d[T2] - v2 * total, a + b, d[SC] - z * a]

    return split


def assemble(wave, mean):
    species = [wave(k) for k in range(NS)]
    slow, shear1, shear2, fast, scalar = [wave(k) for k in range(NS, NVAR)]
    y, phi = mean[CY : CY + NS], mean[CPHI : CPHI + NS]
    vn, v1, v2 = mean[CU : CU + 3]
    acoustic = slow + fast
    half_acoustic = 0.5 * acoustic
    pull = mean[CC] * (fast - slow)
    carried = functools.reduce(lambda s, n: s + n, species, acoustic)
    energy = (
        (mean[FWEIGHT] * acoustic - dot(species, phi)) * mean[FINV]
        + mean[FSQUARE] * carried
        + vn * pull
        + v1 * shear1
        + v2 * shear2
    )
    rows = [species[k] + y[k] * half_acoustic for k in range(NS)]
    rows += [vn * carried + pull, v1 * carried + shear1, v2 * carried + shear2, energy]
    return rows + [mean[CZ] * half_acoustic + scalar]


def prepare(first, f, i, uq, cq, lf, lu, bf, bu, mean_ref, places=(0, 1, 2, 3, 4), linear=True, fresh=True):
    if fresh:
        mean = face_means(first, f, cq)
        for n in range(NFACE):
            mean_ref[i, n] = mean[n]
    else:
        mean = [mean_ref[i, n] for n in range(NFACE)]
    split = splitter(mean)
    for n in places:
        here, there = first + f + n, first + f + n + 1
        du = [uq[there, k] - uq[here, k] for k in range(NVAR)]
        df = [cq[there, CF + k] - cq[here, CF + k] for k in range(NVAR)]
        parts = split(du, cq[there, CRHO] - cq[here, CRHO])
        for k in range(NVAR):
            lu[i, n, k] = parts[k]
        parts = split(df, du[NM])
        for k in range(NVAR):
            lf[i, n, k] = parts[k]
    if not linear:
        return
    for k in range(NVAR):
        f0, f1, f2, f3 = [cq[first + f + n, CF + k] for n in (1, 2, 3, 4)]
        bf[i, k] = 7.0 * (f1 + f2) - (f0 + f3)
    for k in range(NVAR):
        u0, u1, u2, u3 = [uq[first + f + n, k] for n in (1, 2, 3, 4)]
        bu[i, k] = (u3 - u0) - 3.0 * (u2 - u1)


def finish(alpha, i, lf, lu, bf, bu, mean_ref, fx):
    def wave(k):
        l = [lf[i, n, k] for n in range(5)]
        a = [alpha * lu[i, n, k] for n in range(5)]
        plus = correction(*[l[n] + a[n] for n in (0, 1, 2, 3)])
        minus = correction(*[l[n] - a[n] for n in (4, 3, 2, 1)])
        return minus - plus

    rows = assemble(wave, [mean_ref[i, n] for n in range(NFACE)])
    for k in range(NVAR):
        fx[i, k] = (bf[i, k] + alpha * bu[i, k]) + rows[k]


def direct(alpha, first, f, i, uq, cq, fx):
    mean = face_means(first, f, cq)
    split = splitter(mean)
    row = first + f
    plus, minus = [[] for _ in range(4)], [[] for _ in range(4)]
    for k in range(NVAR + 1):
        if k < NVAR:
            l = [cq[row + n, CF + k] for n in range(6)]
            a = [alpha * uq[row + n, k] for n in range(6)]
        else:
            l = [uq[row + n, NM] for n in range(6)]
            a = [alpha * cq[row + n, CRHO] for n in range(6)]
        p = [l[n] + a[n] for n in range(5)]
        m = [l[n] - a[n] for n in range(1, 6)]
        dp = [p[n + 1] - p[n] for n in range(4)]
        dm = [m[n + 1] - m[n] for n in range(4)]
        for n in range(4):
            plus[n].append(dp[n])
            minus[n].append(dm[n])
        if k < NVAR:
            x = dp[2] - dm[1]
            fx[i, k] = 6.0 * (p[2] + m[2]) + ((dp[1] - dm[2]) + (x + x))
    plus = [split(d[:NVAR], d[NVAR]) for d in plus]
    minus = [split(d[:NVAR], d[NVAR]) for d in minus]

    def wave(k):
        return correction(*[minus[n][k] for n in (3, 2, 1, 0)]) - correction(*[plus[n][k] for n in (0, 1, 2, 3)])

    rows = assemble(wave, mean)
    for k in range(NVAR):
        fx[i, k] = fx[i, k] + rows[k]


def kernel(
    u_hbm, nasa_ref, gas_ref, index_ref, kind_ref, out_ref,
    u_ref, u_sem, tab, uq, cq, lf, lu, bf, bu, mean_ref, fx, tmp, alphas,
    mine, slots, halo_send, halo_recv, speed_send, speed_recv,
):
    gx, gy = lax.axis_index("gx"), lax.axis_index("gy")
    nx, ny = lax.axis_size("gx"), lax.axis_size("gy")
    z, y_low, plane, core = gx // 2, gx % 2, gy // 2, gy % 2
    nz, n_plane = nx // 2, ny // 2
    x, y_high = plane // 2, plane % 2
    flat_steps = sorted(
        ((dx, high, low) for dx in range(n_plane // 2) for high in (0, 1) for low in (0, 1)),
        key=lambda d: -min(d[0], n_plane // 2 - d[0]) - (0, 1, 2, 1)[2 * d[1] + d[2]],
    )[:-1]
    tall_steps = sorted(range(1, nz), key=lambda d: -min(d, nz - d))

    def flat(step, sign, to_core):
        dx, high, low = step
        to_low, to_high = (y_low + low) % 2, (y_high + high) % 2
        to_x = (x + sign * dx + n_plane // 2) % (n_plane // 2)
        return (2 * z + to_low, 4 * to_x + 2 * to_high + to_core), 4 * to_x + 2 * to_high + to_low

    def tall(step, sign, to_core):
        to_z = (z + sign * step + nz) % nz
        return (2 * to_z + y_low, 2 * plane + to_core), to_z

    chip = 4 * x + 2 * y_high + y_low
    beside = [
        ((gx + nx - 1 + 2 * y_low) % nx, gy),
        (gx + 1 - 2 * y_low, gy),
        (gx, (gy + 1) % ny),
        (gx, (gy + ny - 1) % ny),
    ]
    load = pltpu.make_async_copy(u_hbm, u_ref, u_sem)
    load.start()
    barrier = pltpu.get_barrier_semaphore()

    def greet(peer):
        pl.semaphore_signal(barrier, inc=1, device_id=peer, device_id_type=MESH)

    @pl.when(core == 1)
    def _():
        for step in flat_steps:
            greet(flat(step, -1, 0)[0])
            greet(flat(step, -1, 1)[0])
        greet((gx, gy - 1))

    for step in tall_steps:
        greet(tall(step, -1, 1)[0])
    for peer in beside:
        greet(peer)

    @pl.when(core == 0)
    def _():
        greet((gx, gy + 1))

    fill_table(nasa_ref, gas_ref, index_ref, tab)
    lane = lax.broadcasted_iota(jnp.int32, (8, 128), 1)
    sub = lax.broadcasted_iota(jnp.int32, (8, 128), 0)
    left = lane < 64
    yb, zb = ROWS, 2 * ROWS

    load.wait()
    for k in range(NVAR):
        for r in range(8):
            uq[3 + r, k] = u_ref[ORDER[0][k], 8 * r : 8 * r + 8, :]

    def cells(r):
        cell = cell_row([uq[r, k] for k in range(NVAR)], tab)
        for n in range(NCELL):
            cq[r, n] = cell[n]

    def speeds_with(r, best):
        speed = speed_row([uq[r, k] for k in range(NVAR)], tab)
        return tuple(jnp.maximum(a, b) for a, b in zip(best, speed))

    zero = jnp.zeros((8, 128), jnp.float32)
    best = lax.fori_loop(
        0, 4, lambda n, best: speeds_with(2 * n + 4, speeds_with(2 * n + 3, best)), (zero, zero, zero)
    )
    row = jnp.zeros((1, 128), jnp.float32)
    for d in range(3):
        row = jnp.where(lane[:1] == d, jnp.max(best[d], keepdims=True), row)
    mine[0] = row

    to_core_1 = len(flat_steps) + 2 * len(tall_steps) + 1 + len(beside)
    to_core_0 = len(flat_steps) + 1 + len(beside)

    @pl.when(core == 1)
    def _():
        pl.semaphore_wait(barrier, to_core_1)

    @pl.when(core == 0)
    def _():
        pl.semaphore_wait(barrier, to_core_0)


    def speed_copy(stage, n, slot, peer):
        return pltpu.make_async_remote_copy(
            src_ref=mine.at[stage],
            dst_ref=slots.at[stage, slot],
            send_sem=speed_send.at[stage, n],
            recv_sem=speed_recv.at[stage, slot],
            device_id=peer,
            device_id_type=MESH,
        )

    partner = (gx, gy + 1 - 2 * core)
    last = len(flat_steps)
    first_copies = [
        speed_copy(0, n, 2 * chip + core, flat(step, 1, 1)[0]) for n, step in enumerate(flat_steps)
    ]
    second_copies = [
        speed_copy(1, 2 * n + to_core, z, tall(step, 1, to_core)[0])
        for n, step in enumerate(tall_steps)
        for to_core in (0, 1)
    ] + [speed_copy(1, last, z, partner)]
    inward = speed_copy(0, last, 2 * chip + core, partner)

    for copy in first_copies:
        copy.start()

    @pl.when(core == 0)
    def _():
        inward.start()

    pieces = (
        (3 + 5 * y_low, 11 - 11 * y_low),
        (8 - 5 * y_low, 11 * y_low),
        (yb + 8, yb),
        (yb + 3, yb + 11),
    )
    halos = [
        pltpu.make_async_remote_copy(
            src_ref=uq.at[pl.ds(source, 3)],
            dst_ref=uq.at[pl.ds(target, 3)],
            send_sem=halo_send.at[n],
            recv_sem=halo_recv.at[n],
            device_id=beside[n],
            device_id_type=MESH,
        )
        for n, (source, target) in enumerate(pieces)
    ]
    halos[0].start()

    for pair in range(NVAR // 2):
        a, b = 2 * pair, 2 * pair + 1
        turned = jnp.transpose(jnp.concatenate([u_ref[a], u_ref[b]], axis=0))
        for t in range(8):
            lo, hi = turned[8 * t : 8 * t + 8], turned[64 + 8 * t : 72 + 8 * t]
            tmp[a, 8 * t : 8 * t + 8, :] = jnp.where(left, lo, pltpu.roll(hi, 64, 1))
            tmp[b, 8 * t : 8 * t + 8, :] = jnp.where(left, pltpu.roll(lo, 64, 1), hi)
    low_wall, high_wall = kind_ref[0, 0, 0] == 1, kind_ref[0, 0, 1] == 1
    for k in range(NVAR):
        cz = ORDER[2][k]
        rows = [tmp[cz, pl.ds(l, 8, stride=8), :] for l in range(8)]
        for l in range(8):
            uq[zb + 3 + l, k] = rows[l]
        sign = -1.0 if k == NM else 1.0
        for n in range(3):
            inside = pltpu.roll(rows[7 - n], 1, 0)
            ghost = jnp.where(low_wall, sign * rows[n], rows[0])
            edge = jnp.where(left, ghost, pltpu.roll(inside, 64, 1))
            uq[zb + 2 - n, k] = jnp.where(sub == 0, edge, inside)
            inside = pltpu.roll(rows[n], 7, 0)
            ghost = jnp.where(high_wall, sign * rows[7 - n], rows[7])
            edge = jnp.where(left, pltpu.roll(inside, 64, 1), ghost)
            uq[zb + 11 + n, k] = jnp.where(sub == 7, edge, inside)

    for k in range(NVAR):
        for r in range(8):
            uq[yb + 3 + r, k] = u_ref[ORDER[1][k], pl.ds(r, 8, stride=8), :]

    def before(first, f, i, *how):
        prepare(first, f, i, uq, cq, lf, lu, bf, bu, mean_ref, *how)

    def rest(d):
        for f, places, linear in ((1, (0, 1), True), (2, (0,), False), (6, (4,), False), (7, (3, 4), True)):
            before(ROWS * d, f, FACES * d + f, places, linear, False)

        @pl.loop(0, 2)
        def _(n):
            direct(alphas[d], ROWS * d, 8 * n, FACES * d + 8 * n, uq, cq, fx)

        @pl.loop(0, 4)
        def _(n):
            after(d, FACES * d + 1 + n + 3 * (n // 2))

    @pl.loop(zb, zb + ROWS)
    def _(r):
        cells(r)

    @pl.loop(yb + 3, yb + 11)
    def _(r):
        cells(r)

    halos[1].start()
    @pl.loop(0, FACES)
    def _(f):
        before(zb, f, 2 * FACES + f)

    @pl.when(core == 1)
    def _():
        places = [2 * flat(step, -1, 1)[1] + side for step in flat_steps for side in (0, 1)] + [2 * chip]
        for slot in places:
            speed_copy(0, 0, slot, partner).wait_recv()
        total = mine[0]
        for slot in places:
            total = jnp.maximum(total, slots[0, slot])
        mine[1] = total
        for copy in second_copies:
            copy.start()
        slots[1, z] = total

    halos[2].start()
    halos[3].start()

    @pl.loop(0, 4)
    def _(n):
        cells(2 * n + 3)
        cells(2 * n + 4)

    @pl.loop(0, 6)
    def _(n):
        d = n // 3
        f = 3 + n - 3 * d
        before(ROWS * d, f, FACES * d + f)

    @pl.loop(0, 2)
    def _(d):
        for f, places, linear in (
            (1, (2, 3, 4), False),
            (2, (1, 2, 3, 4), True),
            (6, (0, 1, 2, 3), True),
            (7, (0, 1, 2), False),
        ):
            before(ROWS * d, f, FACES * d + f, places, linear)

    for step in tall_steps:
        speed_copy(1, 0, tall(step, -1, 1)[1], partner).wait_recv()

    @pl.when(core == 0)
    def _():
        speed_copy(1, 0, z, partner).wait_recv()

    speeds = slots[1, 0]
    for n in range(1, nz):
        speeds = jnp.maximum(speeds, slots[1, n])
    total = None
    for d in range(3):
        alpha = jnp.max(jnp.where(lane[:1] == d, speeds, 0.0), keepdims=True)
        alphas[d] = jnp.broadcast_to(alpha, (8, 128))
        total = alphas[d] if total is None else total + alphas[d]
    scale = (COURANT / 12.0) / total

    def after(d, i):
        finish(alphas[d], i, lf, lu, bf, bu, mean_ref, fx)

    @pl.loop(2 * FACES, 3 * FACES)
    def _(i):
        after(2, i)

    @pl.loop(0, 2)
    def _(d):
        @pl.loop(3, 6)
        def _(f):
            after(d, FACES * d + f)

    halos[0].wait_recv()
    halos[1].wait_recv()

    @pl.loop(0, 3)
    def _(n):
        cells(n)
        cells(n + 11)

    rest(0)

    halos[2].wait_recv()
    halos[3].wait_recv()

    @pl.loop(0, 3)
    def _(n):
        cells(yb + n)
        cells(yb + n + 11)

    rest(1)


    for k in range(NVAR):
        for d, turned in ((1, u_ref), (2, tmp)):
            flux = [fx[d * FACES + r, k] for r in range(FACES)]
            for r in range(8):
                turned[ORDER[d][k], 8 * r : 8 * r + 8, :] = flux[r] - flux[r + 1]
    for pair in range(NVAR // 2):
        a, b = 2 * pair, 2 * pair + 1
        low, high = [], []
        for t in range(8):
            ra = tmp[a, pl.ds(t, 8, stride=8), :]
            rb = tmp[b, pl.ds(t, 8, stride=8), :]
            low.append(jnp.where(left, ra, pltpu.roll(rb, 64, 1)))
            high.append(jnp.where(left, pltpu.roll(ra, 64, 1), rb))
        back = jnp.transpose(jnp.concatenate(low + high, axis=0))
        for k, start in ((a, 0), (b, 64)):
            flux = [fx[r, k] for r in range(FACES)]
            for r in range(8):
                rate = (flux[r] - flux[r + 1]) + u_ref[k, pl.ds(r, 8, stride=8), :]
                out_ref[k, 8 * r : 8 * r + 8] = scale * (rate + back[start + 8 * r : start + 8 * r + 8])

    for copy in halos:
        copy.wait_send()
    for copy in first_copies:
        copy.wait_send()

    @pl.when(core == 0)
    def _():
        inward.wait_send()

    @pl.when(core == 1)
    def _():
        for copy in second_copies:
            copy.wait_send()


def solution(mesh):
    def shards(u, nasa, gas, index, kind):
        vmem = pl.BlockSpec(memory_space=pltpu.VMEM)
        smem = pl.BlockSpec(memory_space=pltpu.SMEM)
        f32 = jnp.float32

        def rows(*lead):
            return pltpu.VMEM(lead + (8, 128), f32)

        out = pl.pallas_call(
            kernel,
            out_shape=jax.ShapeDtypeStruct((NVAR, 64, 128), f32),
            in_specs=[pl.BlockSpec(memory_space=pl.ANY)] + [smem] * 4,
            out_specs=vmem,
            scratch_shapes=[
                pltpu.VMEM((NVAR, 64, 128), f32),
                pltpu.SemaphoreType.DMA,
                pltpu.SMEM((NS, 11), f32),
                rows(3 * ROWS, NVAR),
                rows(3 * ROWS, NCELL),
                rows(3 * FACES, 5, NVAR),
                rows(3 * FACES, 5, NVAR),
                rows(3 * FACES, NVAR),
                rows(3 * FACES, NVAR),
                rows(3 * FACES, NFACE),
                rows(3 * FACES, NVAR),
                pltpu.VMEM((NVAR, 64, 128), f32),
                rows(3),
                pltpu.VMEM((2, 1, 128), f32),
                pltpu.VMEM((2, 32, 1, 128), f32),
                pltpu.SemaphoreType.DMA((4,)),
                pltpu.SemaphoreType.DMA((4,)),
                pltpu.SemaphoreType.DMA((2, 16)),
                pltpu.SemaphoreType.DMA((2, 32)),
            ],
            compiler_params=pltpu.CompilerParams(
                collective_id=0, has_side_effects=True, vmem_limit_bytes=36 * 1024 * 1024
            ),
        )(*[pltpu.with_memory_space_constraint(a, pltpu.HBM) for a in (u.reshape(NVAR, 64, 128), nasa.T, gas, index, kind)])
        return out.reshape(u.shape)

    whole = P(None, "gx", "gy", None)
    return jax.shard_map(
        shards, mesh=mesh, in_specs=(whole, P(), P(), P(), P("gx", "gy", None)), out_specs=whole, check_vma=False
    )
```
